512 devices in a mesh: gx: 32 (over x, y, core), gy: 16 (over z).
Axes of the slice: x: 4, y: 4, z: 16, core: 2. Of those that a mesh axis runs over, the one named last changes fastest.
Arguments:
- node_disp: float32 [2, 1024, 4096], P(None, 'gx', 'gy'), may hold values from -0.24 to 0.24
- node_vel: float32 [2, 1024, 4096], P(None, 'gx', 'gy'), may hold values from -6 to 6
- node_mass: float32 [1024, 4096], P('gx', 'gy'), may hold values from 0.5 to 2
- zone_mass: float32 [1024, 4096], P('gx', 'gy'), may hold values from 0.5 to 2
- zone_energy: float32 [1024, 4096], P('gx', 'gy'), may hold values from 0.3 to 7.5
- master_block: bfloat16 [512, 4, 16384], P(('gx', 'gy')), may hold values from -3 to 3, as said below
- owner: int32 [1], replicated, may hold values from 0 to 511
- pair_node: int32 [512, 1024], P(('gx', 'gy')), may hold values from 0 to 8191
- pair_segment: int32 [512, 1024], P(('gx', 'gy')), may hold values from 0 to 16382
- pair_side: int32 [512, 1024], P(('gx', 'gy')), may hold values 0 or 1
- pair_count: int32 [512], P(('gx', 'gy')), may hold values from 0 to 1024, as said below
Outputs:
- new_vel: float32 [2, 1024, 4096], P(None, 'gx', 'gy')
- new_disp: float32 [2, 1024, 4096], P(None, 'gx', 'gy')
- master_impulse: float32 [3, 16384], P(None, ('gx', 'gy'))
The draws below stay inside these ranges and needn't reach their ends.
Inputs may be any that keep to these rules, and one draw needn't show every extreme that they name: `pair_node`: local node numbers, row-major over a device's 32 x 256 block. `pair_count`: at most 1024; one device has exactly 1024 in every draw; slots at or past a device's count are not pairs. `master_block`: rows 0 and 1 lie within -0.25 to 0.25.
All inputs are finite; a program needn't handle non-finite values. No bound on the sum of `pair_side` on one device may be relied on, other than what follows from the above.
Results may differ from the reference program's by a relative error of at most 0.0015.
Values may be sent and summed in bfloat16 or wider, within the bound.
No kernel may reach another device: no remote copies, remote signals or barrier semaphores. Data moves between devices by JAX's collectives and lax.ppermute only.
A program may use at most 128 MiB of HBM per device.

```python
import jax
import jax.numpy as jnp

CX = 32
CY = 256
MDEV = 32
PAIRS_DEV = 1024
NX = 1024
NY = 4096
MNODES = 16384
N_GX = 32
N_GY = 16


def draw_zone_energy(key, part):
    row_pos = jnp.arange(NX, dtype=jnp.float32)[:, None] / NX
    col_pos = jnp.arange(NY, dtype=jnp.float32)[None, :] / NY
    level = 10.0 ** (0.5 * (row_pos + col_pos))
    factor = jnp.exp(jnp.clip(0.15 * jax.random.normal(key, (NX, NY), jnp.float32), -0.35, 0.35))
    return (0.5 * level * factor).astype(jnp.float32)


def draw_master_block(key, part):
    devices = MNODES // MDEV
    scales = jnp.array([0.08, 0.08, 1.0, 1.0], jnp.float32)[None, :, None]
    values = jax.random.truncated_normal(key, -3.0, 3.0, (devices, 4, MNODES), jnp.float32)
    return (values * scales).astype(jnp.bfloat16)


def draw_pair_segment(key, part):
    devices = MNODES // MDEV
    device_ids = jnp.arange(devices, dtype=jnp.int32)[:, None]
    offsets = jax.random.randint(jax.random.fold_in(key, 11), (devices, PAIRS_DEV), -MDEV, 2 * MDEV, dtype=jnp.int32)
    nearby = jnp.clip(device_ids * MDEV + offsets, 0, MNODES - 2)
    faraway = jax.random.randint(jax.random.fold_in(key, 12), (devices, PAIRS_DEV), 0, MNODES - 1, dtype=jnp.int32)
    picker = jax.random.randint(jax.random.fold_in(key, 13), (devices, PAIRS_DEV), 0, 2, dtype=jnp.int32)
    return jnp.where(picker == 1, faraway, nearby).astype(jnp.int32)


def draw_pair_count(key, part):
    devices = MNODES // MDEV
    first = jax.random.randint(jax.random.fold_in(key, 1), (devices,), 0, PAIRS_DEV + 1, dtype=jnp.int32)
    second = jax.random.randint(jax.random.fold_in(key, 2), (devices,), 0, PAIRS_DEV + 1, dtype=jnp.int32)
    busiest = jax.random.randint(jax.random.fold_in(key, 3), (), 0, devices, dtype=jnp.int32)
    counts = first * second // PAIRS_DEV
    return jnp.where(jnp.arange(devices, dtype=jnp.int32) == busiest, PAIRS_DEV, counts).astype(jnp.int32)


def with_ends(result, stream_key, low, top_value):
    index_at = [jax.random.randint(jax.random.fold_in(stream_key, axis), (), 0, length) for axis, length in enumerate(result.shape)]
    main_axis = result.shape.index(max(result.shape))
    beside = index_at[:main_axis] + [(index_at[main_axis] + 1) % result.shape[main_axis]] + index_at[main_axis + 1:]
    return result.at[tuple(index_at)].set(low).at[tuple(beside)].set(top_value)


def shard_levels(rng, shape, split, least, high):
    factor_of = 1.0
    for dim, blocks in split:
        heights = jax.random.uniform(jax.random.fold_in(jax.random.fold_in(rng, 6), dim), (blocks,), jnp.float32, least / len(split), high / len(split))
        factor_of = factor_of * jnp.repeat(jnp.exp(heights), shape[dim] // blocks).reshape((-1,) + (1,) * (len(shape) - 1 - dim))
    return factor_of


def bell_draw(key, dims, scale, most, pieces=(), kind=jnp.bfloat16):
    values = scale * jax.random.normal(key, dims, jnp.float32)
    if pieces:
        values = values * shard_levels(key, dims, pieces, -0.22, 0.18)
    return jnp.clip(values, -most, most).astype(kind)


def setup_inputs(seed: int = 0) -> dict:
    key_list = jax.random.split(jax.random.key(seed), 12)
    node_disp = bell_draw(key_list[0], (2, NX, NY), 0.08, 0.24, ((1, 32), (2, 16)), jnp.float32)
    node_vel = bell_draw(key_list[1], (2, NX, NY), 1.0, 6.0, ((1, 32), (2, 16)), jnp.float32)
    node_mass = jnp.clip(0.5 + 1.5 * jax.random.uniform(key_list[2], (NX, NY), jnp.float32) ** shard_levels(key_list[2], (NX, NY), ((0, 32), (1, 16)), -0.2, 0.2), 0.5, 2.0)
    zone_mass = jnp.clip(0.5 + 1.5 * jax.random.uniform(key_list[3], (NX, NY), jnp.float32) ** shard_levels(key_list[3], (NX, NY), ((0, 32), (1, 16)), -0.2, 0.2), 0.5, 2.0)
    zone_energy = draw_zone_energy(jax.random.fold_in(key_list[11], 71), 0)
    master_block = draw_master_block(jax.random.fold_in(key_list[11], 71), 0)
    owner = jax.random.randint(key_list[6], (1,), 0, N_GX * N_GY).astype(jnp.int32)
    pair_node = with_ends(jax.random.randint(key_list[7], (N_GX * N_GY, PAIRS_DEV), 0, CX * CY), jax.random.fold_in(key_list[7], 1), 0, (CX * CY) - 1).astype(jnp.int32)
    pair_segment = draw_pair_segment(jax.random.fold_in(key_list[11], 71), 0)
    pair_side = with_ends((jax.random.randint(key_list[9], (N_GX * N_GY, PAIRS_DEV), 0, 2) < 1).astype(jnp.int32), jax.random.fold_in(key_list[9], 1), 0, 1)
    pair_count = draw_pair_count(jax.random.fold_in(key_list[11], 71), 0)
    return {"node_disp": node_disp, "node_vel": node_vel, "node_mass": node_mass, "zone_mass": zone_mass, "zone_energy": zone_energy, "master_block": master_block, "owner": owner, "pair_node": pair_node, "pair_segment": pair_segment, "pair_side": pair_side, "pair_count": pair_count}


STIFFNESS = 10.0
GAP_SCALE = 0.05

def corner_forces(corner_a, corner_b, corner_c, corner_e, zone_load, zone_live):
    first_dx = 1.0 + corner_c[0] - corner_a[0]
    first_dy = 1.0 + corner_c[1] - corner_a[1]
    second_dx = -1.0 + corner_e[0] - corner_b[0]
    second_dy = 1.0 + corner_e[1] - corner_b[1]
    zone_area = 0.5 * (first_dx * second_dy - second_dx * first_dy)
    safe_area = jnp.where(zone_live, zone_area, 1.0)
    half_press = jnp.where(zone_live, 0.2 * zone_load / safe_area, 0.0)
    force_a = jnp.stack([-half_press * second_dy, half_press * second_dx])
    force_b = jnp.stack([half_press * first_dy, -half_press * first_dx])
    return (safe_area, force_a, force_b, -force_a, -force_b)

def contact_terms(slave_disp, seg_start, seg_end, side_flags, live_mask):
    rel_x = slave_disp[0] - seg_start[0] + 0.5
    rel_y = slave_disp[1] - seg_start[1]
    along_x = 1.0 + seg_end[0] - seg_start[0]
    along_y = seg_end[1] - seg_start[1]
    along_sq = along_x * along_x + along_y * along_y
    length = jnp.sqrt(along_sq)
    fraction = (rel_x * along_x + rel_y * along_y) / along_sq
    normal_x = -along_y / length
    normal_y = along_x / length
    gap_size = normal_x * rel_x + normal_y * rel_y
    side_sign = 1.0 - 2.0 * side_flags.astype(jnp.float32)
    magnitude = jnp.where(live_mask, STIFFNESS * GAP_SCALE * jax.nn.softplus(-side_sign * gap_size / GAP_SCALE), 0.0)
    slave_push = jnp.stack([magnitude * side_sign * normal_x, magnitude * side_sign * normal_y])
    react_first = jnp.stack([-(1.0 - fraction) * slave_push[0], -(1.0 - fraction) * slave_push[1], (1.0 - fraction) * magnitude])
    react_second = jnp.stack([-fraction * slave_push[0], -fraction * slave_push[1], fraction * magnitude])
    return (slave_push, react_first, react_second)

def shift_up(values, row_step, col_step):
    padded = jnp.pad(values, ((0, 0), (0, row_step), (0, col_step)))
    return padded[:, row_step:, col_step:]

def shift_down(values, row_step, col_step):
    padded = jnp.pad(values, ((0, 0), (row_step, 0), (col_step, 0)))
    return padded[:, :NX, :NY]

def reference(node_disp, node_vel, node_mass, zone_mass, zone_energy, master_block, owner, pair_node, pair_segment, pair_side, pair_count):
    row_ids = jnp.arange(NX, dtype=jnp.int32)[:, None]
    col_ids = jnp.arange(NY, dtype=jnp.int32)[None, :]
    zone_live = (row_ids < NX - 1) & (col_ids < NY - 1)
    safe_area, force_a, force_b, force_c, force_e = corner_forces(node_disp, shift_up(node_disp, 1, 0), shift_up(node_disp, 1, 1), shift_up(node_disp, 0, 1), zone_energy * zone_mass, zone_live)
    node_force = force_a + shift_down(force_b, 1, 0) + shift_down(force_c, 1, 1) + shift_down(force_e, 0, 1)
    zone_ratio = jnp.where(zone_live, jnp.sqrt(safe_area) / jnp.sqrt(0.56 * zone_energy), 1e+30)
    step_size = 0.3 * jnp.min(zone_ratio)
    surface = master_block[owner[0]].astype(jnp.float32)
    coords = surface[0:2]
    devices = N_GX * N_GY
    rows_dev = NX // N_GX
    cols_dev = NY // N_GY
    device_ids = jnp.arange(devices, dtype=jnp.int32)[:, None]
    node_row = device_ids // N_GY * rows_dev + pair_node // cols_dev
    node_col = device_ids % N_GY * cols_dev + pair_node % cols_dev
    live_mask = jnp.arange(PAIRS_DEV, dtype=jnp.int32)[None, :] < pair_count[:, None]
    slave_disp = node_disp[:, node_row, node_col]
    seg_start = jnp.take(coords, pair_segment, axis=1)
    seg_end = jnp.take(coords, pair_segment + 1, axis=1)
    slave_push, react_first, react_second = contact_terms(slave_disp, seg_start, seg_end, pair_side, live_mask)
    total_force = node_force.at[:, node_row, node_col].add(slave_push)
    reaction = jnp.zeros((3, MNODES), jnp.float32)
    reaction = reaction.at[:, pair_segment].add(react_first).at[:, pair_segment + 1].add(react_second)
    new_vel = node_vel + step_size * total_force / node_mass
    new_disp = node_disp + step_size * new_vel
    master_impulse = jnp.concatenate([surface[2:4] + step_size * reaction[0:2], step_size * reaction[2:3]], axis=0)
    return (new_vel, new_disp, master_impulse)
```

```python
import jax
import jax.numpy as jnp
from jax import lax
from jax.experimental import pallas as pl
from jax.experimental.pallas import tpu as pltpu
from jax.sharding import Mesh
from jax.sharding import PartitionSpec as P

GX = ("gx_0", "gx_1", "gx_2")
GX_GY = ("gx_0", "gx_1", "gx_2", "gy")
NGX = 32
NGY = 16
ROWS = 32
COLS = 256
PAIRS = 1024
TOTAL_ROWS = NGX * ROWS
TOTAL_COLS = NGY * COLS
STIFFNESS = 10.0
GAP_SCALE = 0.05
BLOCK = 256

f32 = jnp.float32
bf16 = jnp.bfloat16
VMEM = pl.BlockSpec(memory_space=pltpu.VMEM)
SMEM = pl.BlockSpec(memory_space=pltpu.SMEM)


def place(ids):
    return ids[0], lax.axis_index(GX), lax.axis_index("gy")


def iota(shape, dim):
    return lax.broadcasted_iota(jnp.int32, shape, dim)


def rows_of(pieces):
    row = iota((8, 128), 0)
    tile = jnp.zeros((8, 128), f32)
    for k, piece in enumerate(pieces):
        tile = jnp.where(row == k, piece, tile)
    return tile


def column_row(columns):
    line, lane = iota((ROWS, 128), 0), iota((ROWS, 128), 1)
    out = jnp.zeros((ROWS, 128), f32)
    for c, column in enumerate(columns):
        out = jnp.where(lane == line + 32 * c, column, out)
    return jnp.sum(out, axis=0, keepdims=True)


def spread_kernel(ids, recv, disp, energy, mass, out):
    owner, _, gy = place(ids)
    chunk = recv[owner // NGY].astype(f32)
    coords = rows_of([chunk[r, c : c + 1] for c in range(2) for r in range(4)])

    def edge(at):
        cut = slice(at, at + 1)
        return column_row([disp[0, :, cut], disp[1, :, cut], energy[:, cut] * mass[:, cut]])

    head, tail = edge(0), edge(COLS - 1)
    after = lax.rem(gy + 1, NGY)
    for z in range(NGY):
        line = jnp.where(after == z, tail, head)
        low = rows_of([line, chunk[z // 4, 2:3], chunk[z // 4, 3:4]])
        out[z] = jnp.concatenate([coords, low], axis=0).astype(bf16)


def gather_kernel(ids, recv, disp, energy, mass, out, sides, impulse):
    owner, gx, gy = place(ids)
    picked = recv[lax.rem(owner, NGY)].astype(f32)
    left = recv[lax.rem(gy + NGY - 1, NGY)].astype(f32)[8:9]
    right = recv[lax.rem(gy + 1, NGY)].astype(f32)[8:9]
    coords = picked[0:8]
    sides[...] = rows_of([left, right])
    impulse[...] = rows_of([picked[9:10], picked[10:11]])

    def edge(at):
        cut = slice(at, at + 1)
        fields = (disp[0, cut], disp[1, cut], energy[cut] * mass[cut])
        return rows_of([f[:, h : h + 128] for f in fields for h in (0, 128)] + [left, right])

    tail = jnp.concatenate([coords, edge(ROWS - 1)], axis=0).astype(bf16)
    head = jnp.concatenate([coords, edge(0)], axis=0).astype(bf16)
    for d in range(NGX):
        out[d] = head
    out[lax.rem(gx + 1, NGX)] = tail


def zone_forces(ids, recv, sides, disp, energy, mass, field, force):
    _, gx, gy = place(ids)
    above = recv[lax.rem(gx + NGX - 1, NGX)].astype(f32)[8:16]
    below = recv[lax.rem(gx + 1, NGX)].astype(f32)[8:16]
    row8, lane8 = iota((8, 128), 0), iota((8, 128), 1)
    line, lane = iota((ROWS, 128), 0), iota((ROWS, 128), 1)
    lane1 = iota((1, 128), 1)

    def corner(rows, k, at):
        return jnp.sum(jnp.where(lane1 == at, rows[k : k + 1], 0.0), axis=1, keepdims=True)

    for c in range(3):
        own = energy[...] * mass[...] if c == 2 else disp[c]
        field[c, 0:ROWS, 0:COLS] = own
        for h in range(2):
            k = 2 * c + h
            field[c, ROWS : ROWS + 8, 128 * h : 128 * h + 128] = jnp.where(
                row8 == 0, below[k : k + 1], jnp.where(row8 == 7, above[k : k + 1], 0.0)
            )
        cols = [
            jnp.sum(jnp.where(lane == line + 32 * c, sides[k : k + 1], 0.0), axis=1, keepdims=True)
            for k in range(2)
        ]
        field[c, 0:ROWS, COLS : COLS + 128] = jnp.where(
            lane == 0, cols[1], jnp.where(lane == 127, cols[0], 0.0)
        )
        first, last = 32 * c, 32 * c + 31
        low = jnp.where(
            lane8 == 0, corner(below, 7, first), jnp.where(lane8 == 127, corner(below, 6, first), 0.0)
        )
        high = jnp.where(
            lane8 == 0, corner(above, 7, last), jnp.where(lane8 == 127, corner(above, 6, last), 0.0)
        )
        field[c, ROWS : ROWS + 8, COLS : COLS + 128] = jnp.where(
            row8 == 0, low, jnp.where(row8 == 7, high, 0.0)
        )

    height, width = ROWS + 8, COLS + 128

    def next_row(v):
        return pltpu.roll(v, height - 1, 0)

    def next_col(v):
        return pltpu.roll(v, width - 1, 1)

    def prev_row(v):
        return pltpu.roll(v, 1, 0)

    def prev_col(v):
        return pltpu.roll(v, 1, 1)

    first, second = [], []
    for c in range(2):
        a = field[c]
        b = next_row(a)
        first.append(next_col(b) - a + 1.0)
        second.append(next_col(a) - b + (-1.0 if c == 0 else 1.0))
    at_row, at_col = iota((height, width), 0), iota((height, width), 1)
    zone_row = jnp.where(at_row == height - 1, -1, at_row)
    zone_col = jnp.where(at_col == width - 1, -1, at_col)
    in_row, in_col = gx * ROWS + zone_row, gy * COLS + zone_col
    live = (
        (zone_row < ROWS)
        & (zone_col < COLS)
        & (in_row >= 0)
        & (in_row < TOTAL_ROWS - 1)
        & (in_col >= 0)
        & (in_col < TOTAL_COLS - 1)
    )
    area = jnp.where(live, 0.5 * (first[0] * second[1] - second[0] * first[1]), 1.0)
    press = jnp.where(live, 0.2 * field[2] / area, 0.0)
    on_a = (-press * second[1], press * second[0])
    on_b = (press * first[1], -press * first[0])
    for c in range(2):
        total = (on_a[c] - prev_col(on_b[c])) + prev_row(on_b[c] - prev_col(on_a[c]))
        force[c] = total[0:ROWS, 0:COLS]
    scale = jnp.where(
        live[0:ROWS, 0:COLS], jnp.sqrt(area[0:ROWS, 0:COLS]) / jnp.sqrt(0.56 * energy[...]), 1e30
    )
    least = jnp.min(scale, axis=0, keepdims=True)
    return jnp.minimum(least[:, 0:128], least[:, 128:256])


def contact_terms(slave_x, slave_y, start_x, start_y, end_x, end_y, side, live):
    rel_x = slave_x - start_x + 0.5
    rel_y = slave_y - start_y
    along_x = 1.0 + end_x - start_x
    along_y = end_y - start_y
    along_sq = along_x * along_x + along_y * along_y
    length = jnp.sqrt(along_sq)
    fraction = (rel_x * along_x + rel_y * along_y) / along_sq
    normal_x = -along_y / length
    normal_y = along_x / length
    gap_size = normal_x * rel_x + normal_y * rel_y
    sign = 1.0 - 2.0 * side.astype(f32)
    depth = -sign * gap_size / GAP_SCALE
    soft = jnp.maximum(depth, 0.0) + jnp.log1p(jnp.exp(-jnp.abs(depth)))
    magnitude = jnp.where(live, STIFFNESS * GAP_SCALE * soft, 0.0)
    return magnitude * sign * normal_x, magnitude * sign * normal_y, magnitude, fraction


def high_low(v):
    high = v.astype(bf16).astype(f32)
    return high, v - high


def contact_kernel(
    ids,
    count,
    recv,
    sides,
    disp,
    energy,
    mass,
    pair_node,
    pair_segment,
    pair_side,
    out,
    force,
    field,
    nodes,
    picks,
    reaction,
    pushed,
):
    least = zone_forces(ids, recv, sides, disp, energy, mass, field, force)
    coords = recv[...].astype(f32)[:, 0:8].reshape(8 * NGX, 128).astype(bf16)
    for c in range(2):
        for h in range(2):
            rest = disp[c, :, 128 * h : 128 * h + 128]
            for k in range(3):
                high, low = high_low(rest)
                at = 128 * k + 64 * c + 32 * h
                nodes[at : at + 32] = high.astype(bf16)
                rest = low
    reaction[...] = jnp.zeros_like(reaction)
    pushed[...] = jnp.zeros_like(pushed)
    live_count = count[0]

    def block(index, carry):
        begin = pl.multiple_of(index * BLOCK, BLOCK)
        cut = (slice(None), pl.ds(begin, BLOCK))
        segment = pair_segment[cut]
        ends = jnp.concatenate([segment, segment + 1], axis=1)
        end_lane = (iota((128, 2 * BLOCK), 0) == (ends & 127)).astype(f32).astype(bf16)
        end_group, end_row = ends >> 9, (ends >> 7) & 3
        looked = jnp.dot(coords, end_lane, preferred_element_type=f32)
        found = jnp.zeros((8, 2 * BLOCK), f32)
        for s in range(NGX):
            found = found + jnp.where(end_group == s, looked[8 * s : 8 * s + 8], 0.0)
        row8 = iota((8, 2 * BLOCK), 0)
        end_x = jnp.sum(jnp.where(row8 == end_row, found, 0.0), axis=0, keepdims=True)
        end_y = jnp.sum(jnp.where(row8 == end_row + 4, found, 0.0), axis=0, keepdims=True)

        node = pair_node[cut]
        node_lane = (iota((128, BLOCK), 0) == (node & 127)).astype(f32).astype(bf16)
        node_mask = iota((64, BLOCK), 0) == (((node >> 7) & 1) * 32 + (node >> 8))
        seen = jnp.dot(nodes[...], node_lane, preferred_element_type=f32)
        seen = (seen[256:384] + seen[128:256]) + seen[0:128]
        slave_x = jnp.sum(jnp.where(node_mask, seen[0:64], 0.0), axis=0, keepdims=True)
        slave_y = jnp.sum(jnp.where(node_mask, seen[64:128], 0.0), axis=0, keepdims=True)

        live = begin + iota((1, BLOCK), 1) < live_count
        push_x, push_y, magnitude, fraction = contact_terms(
            slave_x,
            slave_y,
            end_x[:, :BLOCK],
            end_y[:, :BLOCK],
            end_x[:, BLOCK:],
            end_y[:, BLOCK:],
            pair_side[cut],
            live,
        )
        share = jnp.concatenate([1.0 - fraction, fraction], axis=1)
        terms = [
            share * jnp.concatenate([v, v], axis=1) for v in (-push_x, -push_y, magnitude)
        ]
        row16 = iota((16, 2 * BLOCK), 0)
        stacked = jnp.where(row16 < 4, terms[0], jnp.where(row16 < 8, terms[1], terms[2]))
        stacked = jnp.where((row16 < 12) & ((row16 & 3) == end_row), stacked, 0.0)
        high, low = high_low(stacked)
        for s in range(NGX):
            mine = end_group == s
            picks[16 * s : 16 * s + 16] = jnp.where(mine, high, 0.0).astype(bf16)
            picks[512 + 16 * s : 528 + 16 * s] = jnp.where(mine, low, 0.0).astype(bf16)
        contract = (((1,), (1,)), ((), ()))
        part = lax.dot_general(picks[...], end_lane, contract, preferred_element_type=f32)
        reaction[...] += part[0:512] + part[512:1024]

        rows = [jnp.where(node_mask, half, 0.0) for v in (push_x, push_y) for half in high_low(v)]
        rows = jnp.concatenate([rows[0], rows[2], rows[1], rows[3]], axis=0).astype(bf16)
        part = lax.dot_general(rows, node_lane, contract, preferred_element_type=f32)
        pushed[...] += part[0:128] + part[128:256]
        return carry

    lax.fori_loop(0, (live_count + BLOCK - 1) // BLOCK, block, 0)
    for c in range(2):
        for h in range(2):
            at = 64 * c + 32 * h
            force[c, :, 128 * h : 128 * h + 128] += pushed[at : at + 32]
    row16 = iota((16, 128), 0)
    for s in range(NGX):
        out[s] = jnp.where(row16 == 12, least, reaction[16 * s : 16 * s + 16])


def sum_kernel(recv, out):
    total = recv[0]
    least = recv[0]
    for s in range(1, NGX):
        part = recv[s]
        total = total + part
        least = jnp.minimum(least, part)
    for q in range(4):
        rows = [total[4 * c + q : 4 * c + q + 1] for c in range(3)] + [least[12:13]]
        tile = rows_of(rows)
        for z in range(4 * q, 4 * q + 4):
            out[z] = tile


def step_kernel(recv, impulse, force, vel, disp, mass, new_vel, new_disp, master):
    gy = lax.axis_index("gy")
    finish(gy, recv, impulse, force, vel, disp, mass, new_vel, new_disp, master)


def finish(gy, recv, impulse, force, vel, disp, mass, new_vel, new_disp, master):
    total = recv[0]
    least = recv[0]
    for z in range(1, NGY):
        part = recv[z]
        total = total + part
        least = jnp.minimum(least, part)
    step = 0.3 * jnp.min(least[3:4], axis=1, keepdims=True)
    for c in range(2):
        vel_c = vel[c] + step * force[c] / mass[...]
        new_vel[c] = vel_c
        new_disp[c] = disp[c] + step * vel_c
    shifted = pltpu.roll(impulse[...] + step * total, lax.rem(128 - 32 * lax.rem(gy, 4), 128), 1)
    master[...] = shifted[0:3, 0:32]


def call(kernel, out, ins, scratch=()):
    return pl.pallas_call(
        kernel,
        out_shape=[jax.ShapeDtypeStruct(s, d) for s, d in out],
        in_specs=[SMEM if i == "s" else VMEM for i in ins],
        out_specs=[VMEM] * len(out),
        scratch_shapes=[pltpu.VMEM(s, d) for s, d in scratch],
    )


def exchange(value, axes):
    return lax.all_to_all(value, axes, 0, 0, tiled=True)


def tiles_of(master_block):
    return master_block[0].reshape(4, NGX, 4, 128).transpose(1, 2, 0, 3)


def stages(
    exchange,
    node_disp,
    node_vel,
    node_mass,
    zone_mass,
    zone_energy,
    master_block,
    owner,
    pair_node,
    pair_segment,
    pair_side,
    pair_count,
):
    fields = (node_disp, zone_energy, zone_mass)
    tiles = exchange(tiles_of(master_block), GX)
    (sent,) = call(spread_kernel, [((NGY, 16, 128), bf16)], "svvvv")(owner, tiles, *fields)
    sent = exchange(sent, "gy")
    sent, sides, impulse = call(
        gather_kernel,
        [((NGX, 16, 128), bf16), ((8, 128), f32), ((8, 128), f32)],
        "svvvv",
    )(owner, sent, *fields)
    sent = exchange(sent, GX)
    sent, force = call(
        contact_kernel,
        [((NGX, 16, 128), f32), ((2, ROWS, COLS), f32)],
        "ssvvvvvvvv",
        [
            ((3, ROWS + 8, COLS + 128), f32),
            ((384, 128), bf16),
            ((1024, 2 * BLOCK), bf16),
            ((512, 128), f32),
            ((128, 128), f32),
        ],
    )(owner, pair_count, sent, sides, *fields, pair_node, pair_segment, pair_side)
    sent = exchange(sent, GX)
    (sent,) = call(sum_kernel, [((NGY, 8, 128), f32)], "v")(sent)
    sent = exchange(sent, "gy")
    return tuple(
        call(
            step_kernel,
            [((2, ROWS, COLS), f32), ((2, ROWS, COLS), f32), ((3, 32), f32)],
            "vvvvvv",
        )(sent, impulse, force, node_vel, node_disp, node_mass)
    )


def shards(*args):
    return stages(exchange, *args)


def solution(mesh):
    split = Mesh(mesh.devices.reshape(4, 4, 2, mesh.shape["gy"]), ("gx_0", "gx_1", "gx_2", "gy"))
    in_specs = (
        P(None, GX, "gy"),
        P(None, GX, "gy"),
        P(GX, "gy"),
        P(GX, "gy"),
        P(GX, "gy"),
        P(GX_GY, None, None),
        P(),
        P(GX_GY, None),
        P(GX_GY, None),
        P(GX_GY, None),
        P(GX_GY),
    )
    out_specs = (P(None, GX, "gy"), P(None, GX, "gy"), P(None, GX_GY))
    return jax.shard_map(
        shards, mesh=split, in_specs=in_specs, out_specs=out_specs, check_vma=False
    )
```

```python
import jax
import jax.numpy as jnp
from jax import lax
from jax.experimental import pallas as pl
from jax.experimental.pallas import tpu as pltpu
from jax.sharding import Mesh
from jax.sharding import PartitionSpec as P

GX = ("gx_0", "gx_1", "gx_2")
GX_GY = ("gx_0", "gx_1", "gx_2", "gy")
NGX = 32
NGY = 16
ROWS = 32
COLS = 256
PAIRS = 1024
TOTAL_ROWS = NGX * ROWS
TOTAL_COLS = NGY * COLS
STIFFNESS = 10.0
GAP_SCALE = 0.05
BLOCK = 256

f32 = jnp.float32
bf16 = jnp.bfloat16
VMEM = pl.BlockSpec(memory_space=pltpu.VMEM)
SMEM = pl.BlockSpec(memory_space=pltpu.SMEM)


def place(ids):
    return ids[0], lax.axis_index(GX), lax.axis_index("gy")


def iota(shape, dim):
    return lax.broadcasted_iota(jnp.int32, shape, dim)


def rows_of(pieces):
    row = iota((8, 128), 0)
    tile = jnp.zeros((8, 128), f32)
    for k, piece in enumerate(pieces):
        tile = jnp.where(row == k, piece, tile)
    return tile


def column_row(columns):
    line, lane = iota((ROWS, 128), 0), iota((ROWS, 128), 1)
    out = jnp.zeros((ROWS, 128), f32)
    for c, column in enumerate(columns):
        out = jnp.where(lane == line + 32 * c, column, out)
    return jnp.sum(out, axis=0, keepdims=True)


def spread_kernel(ids, recv, disp, energy, mass, out):
    owner, _, gy = place(ids)
    chunk = recv[owner // NGY].astype(f32)
    coords = rows_of([chunk[r, c : c + 1] for c in range(2) for r in range(4)])

    def edge(at):
        cut = slice(at, at + 1)
        return column_row([disp[0, :, cut], disp[1, :, cut], energy[:, cut] * mass[:, cut]])

    head, tail = edge(0), edge(COLS - 1)
    after = lax.rem(gy + 1, NGY)
    for z in range(NGY):
        line = jnp.where(after == z, tail, head)
        low = rows_of([line, chunk[z // 4, 2:3], chunk[z // 4, 3:4]])
        out[z] = jnp.concatenate([coords, low], axis=0).astype(bf16)


def gather_kernel(ids, recv, disp, energy, mass, out, sides, impulse):
    owner, gx, gy = place(ids)
    picked = recv[lax.rem(owner, NGY)].astype(f32)
    left = recv[lax.rem(gy + NGY - 1, NGY)].astype(f32)[8:9]
    right = recv[lax.rem(gy + 1, NGY)].astype(f32)[8:9]
    coords = picked[0:8]
    sides[...] = rows_of([left, right])
    impulse[...] = rows_of([picked[9:10], picked[10:11]])

    def edge(at):
        cut = slice(at, at + 1)
        fields = (disp[0, cut], disp[1, cut], energy[cut] * mass[cut])
        return rows_of([f[:, h : h + 128] for f in fields for h in (0, 128)] + [left, right])

    tail = jnp.concatenate([coords, edge(ROWS - 1)], axis=0).astype(bf16)
    head = jnp.concatenate([coords, edge(0)], axis=0).astype(bf16)
    for d in range(NGX):
        out[d] = head
    out[lax.rem(gx + 1, NGX)] = tail


def zone_forces(ids, recv, sides, disp, energy, mass, field, force):
    _, gx, gy = place(ids)
    above = recv[lax.rem(gx + NGX - 1, NGX)].astype(f32)[8:16]
    below = recv[lax.rem(gx + 1, NGX)].astype(f32)[8:16]
    row8, lane8 = iota((8, 128), 0), iota((8, 128), 1)
    line, lane = iota((ROWS, 128), 0), iota((ROWS, 128), 1)
    lane1 = iota((1, 128), 1)

    def corner(rows, k, at):
        return jnp.sum(jnp.where(lane1 == at, rows[k : k + 1], 0.0), axis=1, keepdims=True)

    for c in range(3):
        own = energy[...] * mass[...] if c == 2 else disp[c]
        field[c, 0:ROWS, 0:COLS] = own
        for h in range(2):
            k = 2 * c + h
            field[c, ROWS : ROWS + 8, 128 * h : 128 * h + 128] = jnp.where(
                row8 == 0, below[k : k + 1], jnp.where(row8 == 7, above[k : k + 1], 0.0)
            )
        cols = [
            jnp.sum(jnp.where(lane == line + 32 * c, sides[k : k + 1], 0.0), axis=1, keepdims=True)
            for k in range(2)
        ]
        field[c, 0:ROWS, COLS : COLS + 128] = jnp.where(
            lane == 0, cols[1], jnp.where(lane == 127, cols[0], 0.0)
        )
        first, last = 32 * c, 32 * c + 31
        low = jnp.where(
            lane8 == 0, corner(below, 7, first), jnp.where(lane8 == 127, corner(below, 6, first), 0.0)
        )
        high = jnp.where(
            lane8 == 0, corner(above, 7, last), jnp.where(lane8 == 127, corner(above, 6, last), 0.0)
        )
        field[c, ROWS : ROWS + 8, COLS : COLS + 128] = jnp.where(
            row8 == 0, low, jnp.where(row8 == 7, high, 0.0)
        )

    height, width = ROWS + 8, COLS + 128

    def next_row(v):
        return pltpu.roll(v, height - 1, 0)

    def next_col(v):
        return pltpu.roll(v, width - 1, 1)

    def prev_row(v):
        return pltpu.roll(v, 1, 0)

    def prev_col(v):
        return pltpu.roll(v, 1, 1)

    first, second = [], []
    for c in range(2):
        a = field[c]
        b = next_row(a)
        first.append(next_col(b) - a + 1.0)
        second.append(next_col(a) - b + (-1.0 if c == 0 else 1.0))
    at_row, at_col = iota((height, width), 0), iota((height, width), 1)
    zone_row = jnp.where(at_row == height - 1, -1, at_row)
    zone_col = jnp.where(at_col == width - 1, -1, at_col)
    in_row, in_col = gx * ROWS + zone_row, gy * COLS + zone_col
    live = (
        (zone_row < ROWS)
        & (zone_col < COLS)
        & (in_row >= 0)
        & (in_row < TOTAL_ROWS - 1)
        & (in_col >= 0)
        & (in_col < TOTAL_COLS - 1)
    )
    area = jnp.where(live, 0.5 * (first[0] * second[1] - second[0] * first[1]), 1.0)
    press = jnp.where(live, 0.2 * field[2] / area, 0.0)
    on_a = (-press * second[1], press * second[0])
    on_b = (press * first[1], -press * first[0])
    for c in range(2):
        total = (on_a[c] - prev_col(on_b[c])) + prev_row(on_b[c] - prev_col(on_a[c]))
        force[c] = total[0:ROWS, 0:COLS]
    scale = jnp.where(
        live[0:ROWS, 0:COLS], jnp.sqrt(area[0:ROWS, 0:COLS]) / jnp.sqrt(0.56 * energy[...]), 1e30
    )
    least = jnp.min(scale, axis=0, keepdims=True)
    return jnp.minimum(least[:, 0:128], least[:, 128:256])


def contact_terms(slave_x, slave_y, start_x, start_y, end_x, end_y, side, live):
    rel_x = slave_x - start_x + 0.5
    rel_y = slave_y - start_y
    along_x = 1.0 + end_x - start_x
    along_y = end_y - start_y
    along_sq = along_x * along_x + along_y * along_y
    length = jnp.sqrt(along_sq)
    fraction = (rel_x * along_x + rel_y * along_y) / along_sq
    normal_x = -along_y / length
    normal_y = along_x / length
    gap_size = normal_x * rel_x + normal_y * rel_y
    sign = 1.0 - 2.0 * side.astype(f32)
    depth = -sign * gap_size / GAP_SCALE
    soft = jnp.maximum(depth, 0.0) + jnp.log1p(jnp.exp(-jnp.abs(depth)))
    magnitude = jnp.where(live, STIFFNESS * GAP_SCALE * soft, 0.0)
    return magnitude * sign * normal_x, magnitude * sign * normal_y, magnitude, fraction


def high_low(v):
    high = v.astype(bf16).astype(f32)
    return high, v - high


def contact_kernel(
    ids,
    count,
    recv,
    sides,
    disp,
    energy,
    mass,
    pair_node,
    pair_segment,
    pair_side,
    out,
    force,
    field,
    nodes,
    picks,
    reaction,
    pushed,
):
    least = zone_forces(ids, recv, sides, disp, energy, mass, field, force)
    coords = recv[...].astype(f32)[:, 0:8].reshape(8 * NGX, 128).astype(bf16)
    for c in range(2):
        for h in range(2):
            rest = disp[c, :, 128 * h : 128 * h + 128]
            for k in range(3):
                high, low = high_low(rest)
                at = 128 * k + 64 * c + 32 * h
                nodes[at : at + 32] = high.astype(bf16)
                rest = low
    reaction[...] = jnp.zeros_like(reaction)
    pushed[...] = jnp.zeros_like(pushed)
    live_count = count[0]

    def block(index, carry):
        begin = pl.multiple_of(index * BLOCK, BLOCK)
        cut = (slice(None), pl.ds(begin, BLOCK))
        segment = pair_segment[cut]
        ends = jnp.concatenate([segment, segment + 1], axis=1)
        end_lane = (iota((128, 2 * BLOCK), 0) == (ends & 127)).astype(f32).astype(bf16)
        end_group, end_row = ends >> 9, (ends >> 7) & 3
        looked = jnp.dot(coords, end_lane, preferred_element_type=f32)
        found = jnp.zeros((8, 2 * BLOCK), f32)
        for s in range(NGX):
            found = found + jnp.where(end_group == s, looked[8 * s : 8 * s + 8], 0.0)
        row8 = iota((8, 2 * BLOCK), 0)
        end_x = jnp.sum(jnp.where(row8 == end_row, found, 0.0), axis=0, keepdims=True)
        end_y = jnp.sum(jnp.where(row8 == end_row + 4, found, 0.0), axis=0, keepdims=True)

        node = pair_node[cut]
        node_lane = (iota((128, BLOCK), 0) == (node & 127)).astype(f32).astype(bf16)
        node_mask = iota((64, BLOCK), 0) == (((node >> 7) & 1) * 32 + (node >> 8))
        seen = jnp.dot(nodes[...], node_lane, preferred_element_type=f32)
        seen = (seen[256:384] + seen[128:256]) + seen[0:128]
        slave_x = jnp.sum(jnp.where(node_mask, seen[0:64], 0.0), axis=0, keepdims=True)
        slave_y = jnp.sum(jnp.where(node_mask, seen[64:128], 0.0), axis=0, keepdims=True)

        live = begin + iota((1, BLOCK), 1) < live_count
        push_x, push_y, magnitude, fraction = contact_terms(
            slave_x,
            slave_y,
            end_x[:, :BLOCK],
            end_y[:, :BLOCK],
            end_x[:, BLOCK:],
            end_y[:, BLOCK:],
            pair_side[cut],
            live,
        )
        share = jnp.concatenate([1.0 - fraction, fraction], axis=1)
        terms = [
            share * jnp.concatenate([v, v], axis=1) for v in (-push_x, -push_y, magnitude)
        ]
        row16 = iota((16, 2 * BLOCK), 0)
        stacked = jnp.where(row16 < 4, terms[0], jnp.where(row16 < 8, terms[1], terms[2]))
        stacked = jnp.where((row16 < 12) & ((row16 & 3) == end_row), stacked, 0.0)
        high, low = high_low(stacked)
        for s in range(NGX):
            mine = end_group == s
            picks[16 * s : 16 * s + 16] = jnp.where(mine, high, 0.0).astype(bf16)
            picks[512 + 16 * s : 528 + 16 * s] = jnp.where(mine, low, 0.0).astype(bf16)
        contract = (((1,), (1,)), ((), ()))
        part = lax.dot_general(picks[...], end_lane, contract, preferred_element_type=f32)
        reaction[...] += part[0:512] + part[512:1024]

        rows = [jnp.where(node_mask, half, 0.0) for v in (push_x, push_y) for half in high_low(v)]
        rows = jnp.concatenate([rows[0], rows[2], rows[1], rows[3]], axis=0).astype(bf16)
        part = lax.dot_general(rows, node_lane, contract, preferred_element_type=f32)
        pushed[...] += part[0:128] + part[128:256]
        return carry

    lax.fori_loop(0, (live_count + BLOCK - 1) // BLOCK, block, 0)
    for c in range(2):
        for h in range(2):
            at = 64 * c + 32 * h
            force[c, :, 128 * h : 128 * h + 128] += pushed[at : at + 32]
    row16 = iota((16, 128), 0)
    for s in range(NGX):
        out[s] = jnp.where(row16 == 12, least, reaction[16 * s : 16 * s + 16])


def sum_kernel(recv, out):
    total = recv[0]
    least = recv[0]
    for s in range(1, NGX):
        part = recv[s]
        total = total + part
        least = jnp.minimum(least, part)
    for q in range(4):
        rows = [total[4 * c + q : 4 * c + q + 1] for c in range(3)] + [least[12:13]]
        tile = rows_of(rows)
        for z in range(4 * q, 4 * q + 4):
            out[z] = tile


def step_kernel(recv, impulse, force, vel, disp, mass, new_vel, new_disp, master):
    gy = lax.axis_index("gy")
    finish(gy, recv, impulse, force, vel, disp, mass, new_vel, new_disp, master)


def finish(gy, recv, impulse, force, vel, disp, mass, new_vel, new_disp, master):
    total = recv[0]
    least = recv[0]
    for z in range(1, NGY):
        part = recv[z]
        total = total + part
        least = jnp.minimum(least, part)
    step = 0.3 * jnp.min(least[3:4], axis=1, keepdims=True)
    for c in range(2):
        vel_c = vel[c] + step * force[c] / mass[...]
        new_vel[c] = vel_c
        new_disp[c] = disp[c] + step * vel_c
    shifted = pltpu.roll(impulse[...] + step * total, lax.rem(128 - 32 * lax.rem(gy, 4), 128), 1)
    master[...] = shifted[0:3, 0:32]


def call(kernel, out, ins, scratch=()):
    return pl.pallas_call(
        kernel,
        out_shape=[jax.ShapeDtypeStruct(s, d) for s, d in out],
        in_specs=[SMEM if i == "s" else VMEM for i in ins],
        out_specs=[VMEM] * len(out),
        scratch_shapes=[pltpu.VMEM(s, d) for s, d in scratch],
        compiler_params=pltpu.CompilerParams(vmem_limit_bytes=16 << 20),
    )


def exchange(value, axes):
    return lax.all_to_all(value, axes, 0, 0, tiled=True)


def tiles_of(master_block):
    return master_block[0].reshape(4, NGX, 4, 128).transpose(1, 2, 0, 3)


def stages(
    exchange,
    node_disp,
    node_vel,
    node_mass,
    zone_mass,
    zone_energy,
    master_block,
    owner,
    pair_node,
    pair_segment,
    pair_side,
    pair_count,
):
    fields = (node_disp, zone_energy, zone_mass)
    tiles = exchange(tiles_of(master_block), GX)
    (sent,) = call(spread_kernel, [((NGY, 16, 128), bf16)], "svvvv")(owner, tiles, *fields)
    sent = exchange(sent, "gy")
    sent, sides, impulse = call(
        gather_kernel,
        [((NGX, 16, 128), bf16), ((8, 128), f32), ((8, 128), f32)],
        "svvvv",
    )(owner, sent, *fields)
    sent = exchange(sent, GX)
    sent, force = call(
        contact_kernel,
        [((NGX, 16, 128), f32), ((2, ROWS, COLS), f32)],
        "ssvvvvvvvv",
        [
            ((3, ROWS + 8, COLS + 128), f32),
            ((384, 128), bf16),
            ((1024, 2 * BLOCK), bf16),
            ((512, 128), f32),
            ((128, 128), f32),
        ],
    )(owner, pair_count, sent, sides, *fields, pair_node, pair_segment, pair_side)
    sent = exchange(sent, GX)
    (sent,) = call(sum_kernel, [((NGY, 8, 128), f32)], "v")(sent)
    sent = exchange(sent, "gy")
    return tuple(
        call(
            step_kernel,
            [((2, ROWS, COLS), f32), ((2, ROWS, COLS), f32), ((3, 32), f32)],
            "vvvvvv",
        )(sent, impulse, force, node_vel, node_disp, node_mass)
    )


def shards(*args):
    return stages(exchange, *args)


def solution(mesh):
    split = Mesh(mesh.devices.reshape(4, 4, 2, mesh.shape["gy"]), ("gx_0", "gx_1", "gx_2", "gy"))
    in_specs = (
        P(None, GX, "gy"),
        P(None, GX, "gy"),
        P(GX, "gy"),
        P(GX, "gy"),
        P(GX, "gy"),
        P(GX_GY, None, None),
        P(),
        P(GX_GY, None),
        P(GX_GY, None),
        P(GX_GY, None),
        P(GX_GY),
    )
    out_specs = (P(None, GX, "gy"), P(None, GX, "gy"), P(None, GX_GY))
    return jax.shard_map(
        shards, mesh=split, in_specs=in_specs, out_specs=out_specs, check_vma=False
    )
```

```python
import jax
import jax.numpy as jnp
from jax import lax
from jax.experimental import pallas as pl
from jax.experimental.pallas import tpu as pltpu
from jax.sharding import Mesh
from jax.sharding import PartitionSpec as P

GX = ("gx_0", "gx_1", "gx_2")
GX_GY = ("gx_0", "gx_1", "gx_2", "gy")
NGX = 32
NGY = 16
ROWS = 32
COLS = 256
PAIRS = 1024
TOTAL_ROWS = NGX * ROWS
TOTAL_COLS = NGY * COLS
STIFFNESS = 10.0
GAP_SCALE = 0.05
BLOCK = 256

f32 = jnp.float32
bf16 = jnp.bfloat16
VMEM = pl.BlockSpec(memory_space=pltpu.VMEM)
SMEM = pl.BlockSpec(memory_space=pltpu.SMEM)


def place(ids):
    return ids[0], lax.axis_index(GX), lax.axis_index("gy")


def iota(shape, dim):
    return lax.broadcasted_iota(jnp.int32, shape, dim)


def rows_of(pieces):
    row = iota((8, 128), 0)
    tile = jnp.zeros((8, 128), f32)
    for k, piece in enumerate(pieces):
        tile = jnp.where(row == k, piece, tile)
    return tile


def column_row(columns):
    line, lane = iota((ROWS, 128), 0), iota((ROWS, 128), 1)
    out = jnp.zeros((ROWS, 128), f32)
    for c, column in enumerate(columns):
        out = jnp.where(lane == line + 32 * c, column, out)
    return jnp.sum(out, axis=0, keepdims=True)


def spread_kernel(ids, chunk, disp, energy, mass, out):
    _, _, gy = place(ids)
    for h in range(2):
        rows = [chunk[2 * r + h, c : c + 1].astype(f32) for c in range(2) for r in range(2)]
        coords = rows_of(rows)[0:4].astype(bf16)
        for z in range(NGY):
            out[z, h] = coords

    def edge(at):
        cut = slice(at, at + 1)
        columns = [disp[0, :, cut], disp[1, :, cut], energy[:, cut] * mass[:, cut]]
        return rows_of([column_row(columns)])[0:4].astype(bf16)

    head, tail = edge(0), edge(COLS - 1)
    for z in range(NGY):
        out[z, 2] = head
    out[lax.rem(gy + 1, NGY), 2] = tail


def gather_kernel(ids, recv, disp, energy, mass, out, sides):
    owner, gx, gy = place(ids)
    picked = recv[lax.rem(owner, NGY)].astype(f32)
    left = recv[lax.rem(gy + NGY - 1, NGY), 2].astype(f32)[0:1]
    right = recv[lax.rem(gy + 1, NGY), 2].astype(f32)[0:1]
    coords = jnp.concatenate([picked[0], picked[1]], axis=0)
    sides[...] = rows_of([left, right])

    def edge(at):
        cut = slice(at, at + 1)
        fields = (disp[0, cut], disp[1, cut], energy[cut] * mass[cut])
        return rows_of([f[:, h : h + 128] for f in fields for h in (0, 128)] + [left, right])

    tail = jnp.concatenate([coords, edge(ROWS - 1)], axis=0).astype(bf16)
    head = jnp.concatenate([coords, edge(0)], axis=0).astype(bf16)
    for d in range(NGX):
        out[d] = head
    out[lax.rem(gx + 1, NGX)] = tail


def zone_forces(ids, recv, sides, disp, energy, mass, field, force):
    _, gx, gy = place(ids)
    above = recv[lax.rem(gx + NGX - 1, NGX)].astype(f32)[8:16]
    below = recv[lax.rem(gx + 1, NGX)].astype(f32)[8:16]
    row8, lane8 = iota((8, 128), 0), iota((8, 128), 1)
    line, lane = iota((ROWS, 128), 0), iota((ROWS, 128), 1)
    lane1 = iota((1, 128), 1)

    def corner(rows, k, at):
        return jnp.sum(jnp.where(lane1 == at, rows[k : k + 1], 0.0), axis=1, keepdims=True)

    for c in range(3):
        own = energy[...] * mass[...] if c == 2 else disp[c]
        field[c, 0:ROWS, 0:COLS] = own
        for h in range(2):
            k = 2 * c + h
            field[c, ROWS : ROWS + 8, 128 * h : 128 * h + 128] = jnp.where(
                row8 == 0, below[k : k + 1], jnp.where(row8 == 7, above[k : k + 1], 0.0)
            )
        cols = [
            jnp.sum(jnp.where(lane == line + 32 * c, sides[k : k + 1], 0.0), axis=1, keepdims=True)
            for k in range(2)
        ]
        field[c, 0:ROWS, COLS : COLS + 128] = jnp.where(
            lane == 0, cols[1], jnp.where(lane == 127, cols[0], 0.0)
        )
        first, last = 32 * c, 32 * c + 31
        low = jnp.where(
            lane8 == 0, corner(below, 7, first), jnp.where(lane8 == 127, corner(below, 6, first), 0.0)
        )
        high = jnp.where(
            lane8 == 0, corner(above, 7, last), jnp.where(lane8 == 127, corner(above, 6, last), 0.0)
        )
        field[c, ROWS : ROWS + 8, COLS : COLS + 128] = jnp.where(
            row8 == 0, low, jnp.where(row8 == 7, high, 0.0)
        )

    height, width = ROWS + 8, COLS + 128

    def next_row(v):
        return pltpu.roll(v, height - 1, 0)

    def next_col(v):
        return pltpu.roll(v, width - 1, 1)

    def prev_row(v):
        return pltpu.roll(v, 1, 0)

    def prev_col(v):
        return pltpu.roll(v, 1, 1)

    first, second = [], []
    for c in range(2):
        a = field[c]
        b = next_row(a)
        first.append(next_col(b) - a + 1.0)
        second.append(next_col(a) - b + (-1.0 if c == 0 else 1.0))
    at_row, at_col = iota((height, width), 0), iota((height, width), 1)
    zone_row = jnp.where(at_row == height - 1, -1, at_row)
    zone_col = jnp.where(at_col == width - 1, -1, at_col)
    in_row, in_col = gx * ROWS + zone_row, gy * COLS + zone_col
    live = (
        (zone_row < ROWS)
        & (zone_col < COLS)
        & (in_row >= 0)
        & (in_row < TOTAL_ROWS - 1)
        & (in_col >= 0)
        & (in_col < TOTAL_COLS - 1)
    )
    area = jnp.where(live, 0.5 * (first[0] * second[1] - second[0] * first[1]), 1.0)
    press = jnp.where(live, 0.2 * field[2] / area, 0.0)
    on_a = (-press * second[1], press * second[0])
    on_b = (press * first[1], -press * first[0])
    for c in range(2):
        total = (on_a[c] - prev_col(on_b[c])) + prev_row(on_b[c] - prev_col(on_a[c]))
        force[c] = total[0:ROWS, 0:COLS]
    scale = jnp.where(
        live[0:ROWS, 0:COLS], jnp.sqrt(area[0:ROWS, 0:COLS]) / jnp.sqrt(0.56 * energy[...]), 1e30
    )
    return jnp.min(scale, axis=0, keepdims=True)


def contact_terms(slave_x, slave_y, start_x, start_y, end_x, end_y, side, live):
    rel_x = slave_x - start_x + 0.5
    rel_y = slave_y - start_y
    along_x = 1.0 + end_x - start_x
    along_y = end_y - start_y
    along_sq = along_x * along_x + along_y * along_y
    length = jnp.sqrt(along_sq)
    fraction = (rel_x * along_x + rel_y * along_y) / along_sq
    normal_x = -along_y / length
    normal_y = along_x / length
    gap_size = normal_x * rel_x + normal_y * rel_y
    sign = 1.0 - 2.0 * side.astype(f32)
    depth = -sign * gap_size / GAP_SCALE
    soft = jnp.maximum(depth, 0.0) + jnp.log1p(jnp.exp(-jnp.abs(depth)))
    magnitude = jnp.where(live, STIFFNESS * GAP_SCALE * soft, 0.0)
    return magnitude * sign * normal_x, magnitude * sign * normal_y, magnitude, fraction


def high_low(v):
    high = v.astype(bf16).astype(f32)
    return high, v - high


def one_hot(count, index):
    at = lax.broadcasted_iota(jnp.int32, (count, index.shape[1]), 0).astype(f32).astype(bf16)
    return jnp.where(at == index.astype(f32).astype(bf16), jnp.ones((), bf16), jnp.zeros((), bf16))


def blocks_of(live_count):
    return (live_count + BLOCK - 1) // BLOCK


def block_at(index):
    begin = pl.multiple_of(index * BLOCK, BLOCK)
    return begin, (slice(None), pl.ds(begin, BLOCK))


def node_place(node):
    row = ((node >> 7) & 1) * 32 + (node >> 8)
    return one_hot(128, node & 127), iota((64, BLOCK), 0) == row


def slave_kernel(count, disp, pair_node, out, nodes):
    for c in range(2):
        for h in range(2):
            rest = disp[c, :, 128 * h : 128 * h + 128]
            for k in range(3):
                high, low = high_low(rest)
                at = 128 * k + 64 * c + 32 * h
                nodes[at : at + 32] = high.astype(bf16)
                rest = low

    def block(index, carry):
        _, cut = block_at(index)
        lanes, mask = node_place(pair_node[cut])
        seen = jnp.dot(nodes[...], lanes, preferred_element_type=f32)
        seen = (seen[256:384] + seen[128:256]) + seen[0:128]
        for c in range(2):
            found = jnp.where(mask, seen[64 * c : 64 * c + 64], 0.0)
            out[c : c + 1, cut[1]] = jnp.sum(found, axis=0, keepdims=True)
        return carry

    lax.fori_loop(0, blocks_of(count[0]), block, 0)


def contact_kernel(
    ids,
    count,
    recv,
    sides,
    slaves,
    disp,
    energy,
    mass,
    pair_node,
    pair_segment,
    pair_side,
    out,
    force,
    field,
    coords,
    picks,
    reaction,
    pushed,
):
    least = zone_forces(ids, recv, sides, disp, energy, mass, field, force)
    row8 = iota((8, 128), 0)
    for i in range(NGX // 2):
        even, odd = recv[2 * i, 0:8].astype(f32), recv[2 * i + 1, 0:8].astype(f32)
        field[0, 8 * (i % 4) : 8 * (i % 4) + 8, 0:128] = jnp.where(row8 < 4, even, pltpu.roll(odd, 4, 0))
        field[0, 8 * (i % 4) : 8 * (i % 4) + 8, 128:256] = jnp.where(row8 < 4, pltpu.roll(even, 4, 0), odd)
        if i % 4 == 3:
            coords[8 * i - 24 : 8 * i + 8] = field[0, 0:32, 0:256].astype(bf16)
    reaction[...] = jnp.zeros_like(reaction)
    pushed[...] = jnp.zeros_like(pushed)
    live_count = count[0]

    def block(index, carry):
        begin, cut = block_at(index)
        segment = pair_segment[cut]
        ends = jnp.concatenate([segment, segment + 1], axis=1)
        lanes = one_hot(256, ends & 255)
        piece, line = ends >> 9, (ends >> 8) & 1
        looked = jnp.dot(coords[...], lanes, preferred_element_type=f32)
        found = jnp.zeros((8, 2 * BLOCK), f32)
        for s in range(NGX // 2):
            found = found + jnp.where((piece >> 1) == s, looked[8 * s : 8 * s + 8], 0.0)
        row = iota((8, 2 * BLOCK), 0)
        at = (piece & 1) * 4 + line
        end_x = jnp.sum(jnp.where(row == at, found, 0.0), axis=0, keepdims=True)
        end_y = jnp.sum(jnp.where(row == at + 2, found, 0.0), axis=0, keepdims=True)

        live = begin + iota((1, BLOCK), 1) < live_count
        push_x, push_y, magnitude, fraction = contact_terms(
            slaves[0:1, cut[1]],
            slaves[1:2, cut[1]],
            end_x[:, :BLOCK],
            end_y[:, :BLOCK],
            end_x[:, BLOCK:],
            end_y[:, BLOCK:],
            pair_side[cut],
            live,
        )
        push_x, push_y = jnp.where(live, push_x, 0.0), jnp.where(live, push_y, 0.0)
        fraction = jnp.where(live, fraction, 0.0)
        share = jnp.concatenate([1.0 - fraction, fraction], axis=1)
        terms = [
            share * jnp.concatenate([v, v], axis=1) for v in (-push_x, -push_y, magnitude)
        ]
        stacked = jnp.where(row < 2, terms[0], jnp.where(row < 4, terms[1], terms[2]))
        stacked = jnp.where((row < 6) & ((row & 1) == line), stacked, 0.0)
        high, low = high_low(stacked)
        high = jnp.concatenate([high, high], axis=0).astype(bf16)
        low = jnp.concatenate([low, low], axis=0).astype(bf16)
        half = iota((16, 2 * BLOCK), 0) >> 3
        offset = (piece - half).astype(f32).astype(bf16)
        nothing = jnp.zeros((), bf16)
        for s in range(NGX // 2):
            mine = offset == jnp.asarray(2 * s, bf16)
            picks[16 * s : 16 * s + 16] = jnp.where(mine, high, nothing)
            picks[256 + 16 * s : 272 + 16 * s] = jnp.where(mine, low, nothing)
        contract = (((1,), (1,)), ((), ()))
        part = lax.dot_general(picks[...], lanes, contract, preferred_element_type=f32)
        reaction[...] += part[0:256] + part[256:512]

        lanes, mask = node_place(pair_node[cut])
        rows = [jnp.where(mask, half, 0.0) for v in (push_x, push_y) for half in high_low(v)]
        rows = jnp.concatenate([rows[0], rows[2], rows[1], rows[3]], axis=0).astype(bf16)
        part = lax.dot_general(rows, lanes, contract, preferred_element_type=f32)
        pushed[...] += part[0:128] + part[128:256]
        return carry

    lax.fori_loop(0, blocks_of(live_count), block, 0)
    for c in range(2):
        for h in range(2):
            at = 64 * c + 32 * h
            force[c, :, 128 * h : 128 * h + 128] += pushed[at : at + 32]
    row = iota((8, 256), 0)
    for s in range(NGX):
        out[s] = jnp.where(row == 6, least, reaction[8 * s : 8 * s + 8])


def sum_kernel(recv, chunk, out):
    total = recv[0]
    least = recv[0]
    for s in range(1, NGX):
        part = recv[s]
        total = total + part
        least = jnp.minimum(least, part)
    least = jnp.min(least[6:7], axis=1, keepdims=True)
    lane = iota((1, 128), 1)
    for z in range(NGY):
        rows = total[:, 128 * ((z % 8) // 4) : 128 * ((z % 8) // 4) + 128]
        line = jnp.broadcast_to(least, (1, 128))
        old = jnp.zeros((1, 128), f32)
        for c in range(3):
            shift = 32 * ((c - z) % 4)
            mine = (lane >= 32 * c) & (lane < 32 * c + 32)
            row = rows[2 * c + z // 8 : 2 * c + z // 8 + 1]
            line = jnp.where(mine, pltpu.roll(row, shift, 1) if shift else row, line)
            if c < 2:
                row = chunk[z // 4, 2 + c : 3 + c].astype(f32)
                old = jnp.where(mine, pltpu.roll(row, shift, 1) if shift else row, old)
        out[z, 0:1] = line
        out[z, 1:2] = old


def step_kernel(recv, force, vel, disp, mass, new_vel, new_disp, master):
    total = recv[0]
    least = recv[0]
    for z in range(1, NGY):
        part = recv[z]
        total = total + part
        least = jnp.minimum(least, part)
    lane = iota((1, 128), 1)
    least = jnp.where(lane >= 96, least[0:1], 1e30)
    step = 0.3 * jnp.min(least, axis=1, keepdims=True)
    for c in range(2):
        vel_c = vel[c] + step * force[c] / mass[...]
        new_vel[c] = vel_c
        new_disp[c] = disp[c] + step * vel_c
    moved = total[1:2] + step * total[0:1]
    for c in range(3):
        master[c : c + 1, :] = moved[:, 32 * c : 32 * c + 32]


def call(kernel, out, ins, scratch=(), flops=1_000_000):
    return pl.pallas_call(
        kernel,
        out_shape=[jax.ShapeDtypeStruct(s, d) for s, d in out],
        in_specs=[SMEM if i == "s" else VMEM for i in ins],
        out_specs=[VMEM] * len(out),
        scratch_shapes=[pltpu.VMEM(s, d) for s, d in scratch],
        compiler_params=pltpu.CompilerParams(vmem_limit_bytes=16 << 20),
        cost_estimate=pl.CostEstimate(flops=flops, bytes_accessed=1 << 20, transcendentals=0),
    )


def exchange(value, axes):
    return lax.all_to_all(value, axes, 0, 0, tiled=True)


def owner_piece(exchange, master_block, owner):
    def send():
        tiles = master_block[0].reshape(4, NGX, 4, 128).transpose(1, 2, 0, 3)
        return lax.dynamic_index_in_dim(exchange(tiles, GX), owner[0] // NGY, 0, False)

    mine = lax.axis_index("gy") == lax.rem(owner[0], NGY)
    return lax.cond(mine, send, lambda: jnp.zeros((4, 4, 128), bf16))


def stages(
    exchange,
    node_disp,
    node_vel,
    node_mass,
    zone_mass,
    zone_energy,
    master_block,
    owner,
    pair_node,
    pair_segment,
    pair_side,
    pair_count,
):
    fields = (node_disp, zone_energy, zone_mass)
    chunk = owner_piece(exchange, master_block, owner)
    (sent,) = call(spread_kernel, [((NGY, 3, 4, 128), bf16)], "svvvv")(owner, chunk, *fields)
    sent = exchange(sent, "gy")
    sent, sides = call(gather_kernel, [((NGX, 16, 128), bf16), ((8, 128), f32)], "svvvv")(
        owner, sent, *fields
    )
    (slaves,) = call(
        slave_kernel, [((2, PAIRS), f32)], "svv", [((384, 128), bf16)], flops=100_000_000
    )(pair_count, node_disp, pair_node)
    sent = exchange(sent, GX)
    sent, force = call(
        contact_kernel,
        [((NGX, 8, 256), f32), ((2, ROWS, COLS), f32)],
        "ssvvvvvvvvv",
        [
            ((3, ROWS + 8, COLS + 128), f32),
            ((128, 256), bf16),
            ((512, 2 * BLOCK), bf16),
            ((256, 256), f32),
            ((128, 128), f32),
        ],
    )(owner, pair_count, sent, sides, slaves, *fields, pair_node, pair_segment, pair_side)
    sent = exchange(sent, GX)
    (sent,) = call(sum_kernel, [((NGY, 2, 128), f32)], "vv")(sent, chunk)
    sent = exchange(sent, "gy")
    return tuple(
        call(
            step_kernel,
            [((2, ROWS, COLS), f32), ((2, ROWS, COLS), f32), ((3, 32), f32)],
            "vvvvv",
        )(sent, force, node_vel, node_disp, node_mass)
    )


def shards(*args):
    return stages(exchange, *args)


def solution(mesh):
    split = Mesh(mesh.devices.reshape(4, 4, 2, mesh.shape["gy"]), ("gx_0", "gx_1", "gx_2", "gy"))
    in_specs = (
        P(None, GX, "gy"),
        P(None, GX, "gy"),
        P(GX, "gy"),
        P(GX, "gy"),
        P(GX, "gy"),
        P(GX_GY, None, None),
        P(),
        P(GX_GY, None),
        P(GX_GY, None),
        P(GX_GY, None),
        P(GX_GY),
    )
    out_specs = (P(None, GX, "gy"), P(None, GX, "gy"), P(None, GX_GY))
    return jax.shard_map(
        shards, mesh=split, in_specs=in_specs, out_specs=out_specs, check_vma=False
    )
```

```python
import jax
import jax.numpy as jnp
from jax import lax
from jax.experimental import pallas as pl
from jax.experimental.pallas import tpu as pltpu
from jax.sharding import Mesh
from jax.sharding import PartitionSpec as P

GX = ("gx_0", "gx_1", "gx_2")
GX_GY = ("gx_0", "gx_1", "gx_2", "gy")
NGX = 32
NGY = 16
ROWS = 32
COLS = 256
PAIRS = 1024
TOTAL_ROWS = NGX * ROWS
TOTAL_COLS = NGY * COLS
STIFFNESS = 10.0
GAP_SCALE = 0.05

f32 = jnp.float32
bf16 = jnp.bfloat16
VMEM = pl.BlockSpec(memory_space=pltpu.VMEM)
SMEM = pl.BlockSpec(memory_space=pltpu.SMEM)


def place(ids):
    return ids[0], lax.axis_index(GX), lax.axis_index("gy")


def iota(shape, dim):
    return lax.broadcasted_iota(jnp.int32, shape, dim)


def rows_of(pieces):
    row = iota((8, 128), 0)
    tile = jnp.zeros((8, 128), f32)
    for k, piece in enumerate(pieces):
        tile = jnp.where(row == k, piece, tile)
    return tile


def column_row(columns):
    line, lane = iota((ROWS, 128), 0), iota((ROWS, 128), 1)
    out = jnp.zeros((ROWS, 128), f32)
    for c, column in enumerate(columns):
        out = jnp.where(lane == line + 32 * c, column, out)
    return jnp.sum(out, axis=0, keepdims=True)


def edges(gy, disp, energy, mass, out):
    def edge(at):
        cut = slice(at, at + 1)
        columns = [disp[0, :, cut], disp[1, :, cut], energy[:, cut] * mass[:, cut]]
        return rows_of([column_row(columns)])[0:4].astype(bf16)

    head, tail = edge(0), edge(COLS - 1)
    for z in range(NGY):
        out[z, 2] = head
    out[lax.rem(gy + 1, NGY), 2] = tail


def spread_kernel(ids, count, recv, disp, energy, mass, out, extra):
    owner, _, gy = place(ids)
    chunk = recv[owner // NGY].astype(f32)
    for h in range(2):
        rows = [chunk[2 * r + h, c : c + 1] for c in range(2) for r in range(2)]
        coords = rows_of(rows)[0:4].astype(bf16)
        for z in range(NGY):
            out[z, h] = coords
    extra[0:8] = rows_of([chunk[r, 2 + c : 3 + c] for c in range(2) for r in range(4)])
    extra[8:16] = jnp.full((8, 128), count[0].astype(f32))
    edges(gy, disp, energy, mass, out)


def idle_kernel(ids, count, disp, energy, mass, out, extra):
    _, _, gy = place(ids)
    for z in range(NGY):
        out[z] = jnp.zeros((3, 4, 128), bf16)
    extra[0:8] = jnp.zeros((8, 128), f32)
    extra[8:16] = jnp.full((8, 128), count[0].astype(f32))
    edges(gy, disp, energy, mass, out)


def gather_kernel(ids, recv, disp, energy, mass, out, sides):
    owner, gx, gy = place(ids)
    picked = recv[lax.rem(owner, NGY)].astype(f32)
    left = recv[lax.rem(gy + NGY - 1, NGY), 2].astype(f32)[0:1]
    right = recv[lax.rem(gy + 1, NGY), 2].astype(f32)[0:1]
    coords = jnp.concatenate([picked[0], picked[1]], axis=0)
    sides[...] = rows_of([left, right])

    def edge(at):
        cut = slice(at, at + 1)
        fields = (disp[0, cut], disp[1, cut], energy[cut] * mass[cut])
        return rows_of([f[:, h : h + 128] for f in fields for h in (0, 128)] + [left, right])

    tail = jnp.concatenate([coords, edge(ROWS - 1)], axis=0).astype(bf16)
    head = jnp.concatenate([coords, edge(0)], axis=0).astype(bf16)
    for d in range(NGX):
        out[d] = head
    out[lax.rem(gx + 1, NGX)] = tail


def zone_forces(ids, recv, sides, disp, energy, mass, field, force):
    _, gx, gy = place(ids)
    above = recv[lax.rem(gx + NGX - 1, NGX)].astype(f32)[8:16]
    below = recv[lax.rem(gx + 1, NGX)].astype(f32)[8:16]
    row8, lane8 = iota((8, 128), 0), iota((8, 128), 1)
    line, lane = iota((ROWS, 128), 0), iota((ROWS, 128), 1)
    lane1 = iota((1, 128), 1)

    def corner(rows, k, at):
        return jnp.sum(jnp.where(lane1 == at, rows[k : k + 1], 0.0), axis=1, keepdims=True)

    for c in range(3):
        own = energy[...] * mass[...] if c == 2 else disp[c]
        field[c, 0:ROWS, 0:COLS] = own
        for h in range(2):
            k = 2 * c + h
            field[c, ROWS : ROWS + 8, 128 * h : 128 * h + 128] = jnp.where(
                row8 == 0, below[k : k + 1], jnp.where(row8 == 7, above[k : k + 1], 0.0)
            )
        cols = [
            jnp.sum(jnp.where(lane == line + 32 * c, sides[k : k + 1], 0.0), axis=1, keepdims=True)
            for k in range(2)
        ]
        field[c, 0:ROWS, COLS : COLS + 128] = jnp.where(
            lane == 0, cols[1], jnp.where(lane == 127, cols[0], 0.0)
        )
        first, last = 32 * c, 32 * c + 31
        low = jnp.where(
            lane8 == 0, corner(below, 7, first), jnp.where(lane8 == 127, corner(below, 6, first), 0.0)
        )
        high = jnp.where(
            lane8 == 0, corner(above, 7, last), jnp.where(lane8 == 127, corner(above, 6, last), 0.0)
        )
        field[c, ROWS : ROWS + 8, COLS : COLS + 128] = jnp.where(
            row8 == 0, low, jnp.where(row8 == 7, high, 0.0)
        )

    height, width = ROWS + 8, COLS + 128

    def next_row(v):
        return pltpu.roll(v, height - 1, 0)

    def next_col(v):
        return pltpu.roll(v, width - 1, 1)

    def prev_row(v):
        return pltpu.roll(v, 1, 0)

    def prev_col(v):
        return pltpu.roll(v, 1, 1)

    first, second = [], []
    for c in range(2):
        a = field[c]
        b = next_row(a)
        first.append(next_col(b) - a + 1.0)
        second.append(next_col(a) - b + (-1.0 if c == 0 else 1.0))
    at_row, at_col = iota((height, width), 0), iota((height, width), 1)
    zone_row = jnp.where(at_row == height - 1, -1, at_row)
    zone_col = jnp.where(at_col == width - 1, -1, at_col)
    in_row, in_col = gx * ROWS + zone_row, gy * COLS + zone_col
    live = (
        (zone_row < ROWS)
        & (zone_col < COLS)
        & (in_row >= 0)
        & (in_row < TOTAL_ROWS - 1)
        & (in_col >= 0)
        & (in_col < TOTAL_COLS - 1)
    )
    area = jnp.where(live, 0.5 * (first[0] * second[1] - second[0] * first[1]), 1.0)
    press = jnp.where(live, 0.2 * field[2] / area, 0.0)
    on_a = (-press * second[1], press * second[0])
    on_b = (press * first[1], -press * first[0])
    for c in range(2):
        total = (on_a[c] - prev_col(on_b[c])) + prev_row(on_b[c] - prev_col(on_a[c]))
        force[c] = total[0:ROWS, 0:COLS]
    scale = jnp.where(
        live[0:ROWS, 0:COLS], jnp.sqrt(area[0:ROWS, 0:COLS]) / jnp.sqrt(0.56 * energy[...]), 1e30
    )
    return jnp.min(scale, axis=0, keepdims=True)


def contact_terms(slave_x, slave_y, start_x, start_y, end_x, end_y, side, live):
    rel_x = slave_x - start_x + 0.5
    rel_y = slave_y - start_y
    along_x = 1.0 + end_x - start_x
    along_y = end_y - start_y
    along_sq = along_x * along_x + along_y * along_y
    length = jnp.sqrt(along_sq)
    fraction = (rel_x * along_x + rel_y * along_y) / along_sq
    normal_x = -along_y / length
    normal_y = along_x / length
    gap_size = normal_x * rel_x + normal_y * rel_y
    sign = 1.0 - 2.0 * side.astype(f32)
    depth = -sign * gap_size / GAP_SCALE
    soft = jnp.maximum(depth, 0.0) + jnp.log1p(jnp.exp(-jnp.abs(depth)))
    magnitude = jnp.where(live, STIFFNESS * GAP_SCALE * soft, 0.0)
    return magnitude * sign * normal_x, magnitude * sign * normal_y, magnitude, fraction


def high_low(v):
    high = v.astype(bf16).astype(f32)
    return high, v - high


def one_hot(count, index):
    at = lax.broadcasted_iota(jnp.int32, (count, index.shape[1]), 0).astype(f32).astype(bf16)
    return jnp.where(at == index.astype(f32).astype(bf16), jnp.ones((), bf16), jnp.zeros((), bf16))


def node_place(node):
    row = ((node >> 7) & 1) * 32 + (node >> 8)
    return one_hot(128, node & 127), iota((64, PAIRS), 0) == row


def slave_places(disp, pair_node, nodes):
    for c in range(2):
        for h in range(2):
            rest = disp[c, :, 128 * h : 128 * h + 128]
            for k in range(3):
                high, low = high_low(rest)
                at = 128 * k + 64 * c + 32 * h
                nodes[at : at + 32] = high.astype(bf16)
                rest = low
    lanes, mask = node_place(pair_node[...])
    seen = jnp.dot(nodes[...], lanes, preferred_element_type=f32)
    seen = (seen[256:384] + seen[128:256]) + seen[0:128]
    found = [
        jnp.sum(jnp.where(mask, seen[64 * c : 64 * c + 64], 0.0), axis=0, keepdims=True)
        for c in range(2)
    ]
    return found, lanes, mask


def contact_kernel(
    ids,
    extra,
    recv,
    sides,
    disp,
    energy,
    mass,
    pair_node,
    pair_segment,
    pair_side,
    out,
    force,
    field,
    coords,
    nodes,
    picks,
):
    slave, node_lanes, node_mask = slave_places(disp, pair_node, nodes)
    row8 = iota((8, 128), 0)
    for i in range(NGX // 4):
        left, right = [], []
        for s in (4 * i, 4 * i + 2):
            even, odd = recv[s, 0:8].astype(f32), recv[s + 1, 0:8].astype(f32)
            left.append(jnp.where(row8 < 4, even, pltpu.roll(odd, 4, 0)))
            right.append(jnp.where(row8 < 4, pltpu.roll(even, 4, 0), odd))
        coords[16 * i : 16 * i + 16, 0:128] = jnp.concatenate(left, axis=0).astype(bf16)
        coords[16 * i : 16 * i + 16, 128:256] = jnp.concatenate(right, axis=0).astype(bf16)

    segment = pair_segment[...]
    ends = jnp.concatenate([segment, segment + 1], axis=1)
    lanes = one_hot(256, ends & 255)
    piece, line = ends >> 9, (ends >> 8) & 1
    looked = jnp.dot(coords[...], lanes, preferred_element_type=f32)
    found = jnp.zeros((8, 2 * PAIRS), f32)
    for s in range(NGX // 2):
        found = found + jnp.where((piece >> 1) == s, looked[8 * s : 8 * s + 8], 0.0)
    row = iota((8, 2 * PAIRS), 0)
    at = (piece & 1) * 4 + line
    end_x = jnp.sum(jnp.where(row == at, found, 0.0), axis=0, keepdims=True)
    end_y = jnp.sum(jnp.where(row == at + 2, found, 0.0), axis=0, keepdims=True)

    live = iota((1, PAIRS), 1).astype(f32) < extra[8:9, 0:1]
    push_x, push_y, magnitude, fraction = contact_terms(
        slave[0],
        slave[1],
        end_x[:, :PAIRS],
        end_y[:, :PAIRS],
        end_x[:, PAIRS:],
        end_y[:, PAIRS:],
        pair_side[...],
        live,
    )
    share = jnp.concatenate([1.0 - fraction, fraction], axis=1)
    terms = [share * jnp.concatenate([v, v], axis=1) for v in (-push_x, -push_y, magnitude)]
    stacked = jnp.where(row < 2, terms[0], jnp.where(row < 4, terms[1], terms[2]))
    stacked = jnp.where((row < 6) & ((row & 1) == line), stacked, 0.0)
    high, low = high_low(stacked)
    high = jnp.concatenate([high, high], axis=0).astype(bf16)
    low = jnp.concatenate([low, low], axis=0).astype(bf16)
    half = iota((16, 2 * PAIRS), 0) >> 3
    offset = (piece - half).astype(f32).astype(bf16)
    nothing = jnp.zeros((), bf16)
    for s in range(NGX // 2):
        mine = offset == jnp.asarray(2 * s, bf16)
        picks[16 * s : 16 * s + 16] = jnp.where(mine, high, nothing)
        picks[256 + 16 * s : 272 + 16 * s] = jnp.where(mine, low, nothing)
    contract = (((1,), (1,)), ((), ()))
    part = lax.dot_general(picks[...], lanes, contract, preferred_element_type=f32)
    reaction = part[0:256] + part[256:512]

    rows = [jnp.where(node_mask, half, 0.0) for v in (push_x, push_y) for half in high_low(v)]
    rows = jnp.concatenate([rows[0], rows[2], rows[1], rows[3]], axis=0).astype(bf16)
    part = lax.dot_general(rows, node_lanes, contract, preferred_element_type=f32)
    pushed = part[0:128] + part[128:256]

    least = zone_forces(ids, recv, sides, disp, energy, mass, field, force)
    for c in range(2):
        for h in range(2):
            at = 64 * c + 32 * h
            force[c, :, 128 * h : 128 * h + 128] += pushed[at : at + 32]
    row = iota((8, 256), 0)
    for s in range(NGX):
        out[s] = jnp.where(row == 6, least, reaction[8 * s : 8 * s + 8])


def sum_kernel(recv, extra, out):
    total = recv[0]
    least = recv[0]
    for s in range(1, NGX):
        part = recv[s]
        total = total + part
        least = jnp.minimum(least, part)
    least = jnp.min(least[6:7], axis=1, keepdims=True)
    lane = iota((1, 128), 1)
    for z in range(NGY):
        rows = total[:, 128 * ((z % 8) // 4) : 128 * ((z % 8) // 4) + 128]
        line = jnp.broadcast_to(least, (1, 128))
        old = jnp.zeros((1, 128), f32)
        for c in range(3):
            shift = 32 * ((c - z) % 4)
            mine = (lane >= 32 * c) & (lane < 32 * c + 32)
            row = rows[2 * c + z // 8 : 2 * c + z // 8 + 1]
            line = jnp.where(mine, pltpu.roll(row, shift, 1) if shift else row, line)
            if c < 2:
                row = extra[4 * c + z // 4 : 4 * c + z // 4 + 1]
                old = jnp.where(mine, pltpu.roll(row, shift, 1) if shift else row, old)
        out[z, 0:1] = line
        out[z, 1:2] = old


def step_kernel(recv, force, vel, disp, mass, new_vel, new_disp, master):
    total = recv[0]
    least = recv[0]
    for z in range(1, NGY):
        part = recv[z]
        total = total + part
        least = jnp.minimum(least, part)
    lane = iota((1, 128), 1)
    least = jnp.where(lane >= 96, least[0:1], 1e30)
    step = 0.3 * jnp.min(least, axis=1, keepdims=True)
    for c in range(2):
        vel_c = vel[c] + step * force[c] / mass[...]
        new_vel[c] = vel_c
        new_disp[c] = disp[c] + step * vel_c
    moved = total[1:2] + step * total[0:1]
    for c in range(3):
        master[c : c + 1, :] = moved[:, 32 * c : 32 * c + 32]


def call(kernel, out, ins, scratch=(), flops=1_000_000):
    return pl.pallas_call(
        kernel,
        out_shape=[jax.ShapeDtypeStruct(s, d) for s, d in out],
        in_specs=[SMEM if i == "s" else VMEM for i in ins],
        out_specs=[VMEM] * len(out),
        scratch_shapes=[pltpu.VMEM(s, d) for s, d in scratch],
        compiler_params=pltpu.CompilerParams(vmem_limit_bytes=16 << 20),
        cost_estimate=pl.CostEstimate(flops=flops, bytes_accessed=1 << 20, transcendentals=0),
    )


def exchange(value, axes):
    return lax.all_to_all(value, axes, 0, 0, tiled=True)


def owner_piece(exchange, master_block, owner, count, fields):
    tiles = master_block[0].reshape(4, NGX, 4, 128).transpose(1, 2, 0, 3)
    out = [((NGY, 3, 4, 128), bf16), ((16, 128), f32)]

    def send(tiles, owner, count, *fields):
        return tuple(call(spread_kernel, out, "ssvvvv")(owner, count, exchange(tiles, GX), *fields))

    def idle(tiles, owner, count, *fields):
        return tuple(call(idle_kernel, out, "ssvvv")(owner, count, *fields))

    mine = lax.axis_index("gy") == lax.rem(owner[0], NGY)
    return lax.cond(mine, send, idle, tiles, owner, count, *fields)


def stages(
    exchange,
    node_disp,
    node_vel,
    node_mass,
    zone_mass,
    zone_energy,
    master_block,
    owner,
    pair_node,
    pair_segment,
    pair_side,
    pair_count,
):
    fields = (node_disp, zone_energy, zone_mass)
    sent, extra = owner_piece(exchange, master_block, owner, pair_count, fields)
    sent = exchange(sent, "gy")
    sent, sides = call(gather_kernel, [((NGX, 16, 128), bf16), ((8, 128), f32)], "svvvv")(
        owner, sent, *fields
    )
    sent = exchange(sent, GX)
    sent, force = call(
        contact_kernel,
        [((NGX, 8, 256), f32), ((2, ROWS, COLS), f32)],
        "svvvvvvvvv",
        [
            ((3, ROWS + 8, COLS + 128), f32),
            ((128, 256), bf16),
            ((384, 128), bf16),
            ((512, 2 * PAIRS), bf16),
        ],
    )(owner, extra, sent, sides, *fields, pair_node, pair_segment, pair_side)
    sent = exchange(sent, GX)
    (sent,) = call(sum_kernel, [((NGY, 2, 128), f32)], "vv")(sent, extra)
    sent = exchange(sent, "gy")
    return tuple(
        call(
            step_kernel,
            [((2, ROWS, COLS), f32), ((2, ROWS, COLS), f32), ((3, 32), f32)],
            "vvvvv",
        )(sent, force, node_vel, node_disp, node_mass)
    )


def shards(*args):
    return stages(exchange, *args)


def solution(mesh):
    split = Mesh(mesh.devices.reshape(4, 4, 2, mesh.shape["gy"]), ("gx_0", "gx_1", "gx_2", "gy"))
    in_specs = (
        P(None, GX, "gy"),
        P(None, GX, "gy"),
        P(GX, "gy"),
        P(GX, "gy"),
        P(GX, "gy"),
        P(GX_GY, None, None),
        P(),
        P(GX_GY, None),
        P(GX_GY, None),
        P(GX_GY, None),
        P(GX_GY),
    )
    out_specs = (P(None, GX, "gy"), P(None, GX, "gy"), P(None, GX_GY))
    return jax.shard_map(
        shards, mesh=split, in_specs=in_specs, out_specs=out_specs, check_vma=False
    )
```

```python
import jax
import jax.numpy as jnp
from jax import lax
from jax.experimental import pallas as pl
from jax.experimental.pallas import tpu as pltpu
from jax.sharding import Mesh
from jax.sharding import PartitionSpec as P

GX = ("gx_0", "gx_1", "gx_2")
GX_GY = ("gx_0", "gx_1", "gx_2", "gy")
NGX = 32
NGY = 16
ROWS = 32
COLS = 256
PAIRS = 1024
TOTAL_ROWS = NGX * ROWS
TOTAL_COLS = NGY * COLS
STIFFNESS = 10.0
GAP_SCALE = 0.05

f32 = jnp.float32
bf16 = jnp.bfloat16
VMEM = pl.BlockSpec(memory_space=pltpu.VMEM)
SMEM = pl.BlockSpec(memory_space=pltpu.SMEM)


def place(ids):
    return ids[0], lax.axis_index(GX), lax.axis_index("gy")


def iota(shape, dim):
    return lax.broadcasted_iota(jnp.int32, shape, dim)


def rows_of(pieces):
    row = iota((8, 128), 0)
    tile = jnp.zeros((8, 128), f32)
    for k, piece in enumerate(pieces):
        tile = jnp.where(row == k, piece, tile)
    return tile


def column_row(columns):
    line, lane = iota((ROWS, 128), 0), iota((ROWS, 128), 1)
    out = jnp.zeros((ROWS, 128), f32)
    for c, column in enumerate(columns):
        out = jnp.where(lane == line + 32 * c, column, out)
    return jnp.sum(out, axis=0, keepdims=True)


def count_tile(count):
    return jnp.full((8, 128), count[0].astype(f32))


def pick_kernel(owner, count, recv, chunk, tile):
    chunk[...] = recv[owner[0] // NGY]
    tile[...] = count_tile(count)


def idle_kernel(count, chunk, tile):
    chunk[...] = jnp.zeros((4, 4, 128), bf16)
    tile[...] = count_tile(count)


def spread_kernel(chunk, disp, energy, mass, out):
    for h in range(2):
        rows = [chunk[2 * r + h, c : c + 1].astype(f32) for c in range(2) for r in range(2)]
        coords = rows_of(rows)[0:4].astype(bf16)
        for z in range(NGY):
            out[z, h] = coords

    def edge(at):
        cut = slice(at, at + 1)
        columns = [disp[0, :, cut], disp[1, :, cut], energy[:, cut] * mass[:, cut]]
        return rows_of([column_row(columns)])[0:4].astype(bf16)

    head, tail = edge(0), edge(COLS - 1)
    for z in range(NGY):
        out[z, 2] = head
    out[lax.rem(lax.axis_index("gy") + 1, NGY), 2] = tail


def gather_kernel(ids, recv, disp, energy, mass, out, sides):
    owner, gx, gy = place(ids)
    picked = recv[lax.rem(owner, NGY)].astype(f32)
    left = recv[lax.rem(gy + NGY - 1, NGY), 2].astype(f32)[0:1]
    right = recv[lax.rem(gy + 1, NGY), 2].astype(f32)[0:1]
    coords = jnp.concatenate([picked[0], picked[1]], axis=0)
    sides[...] = rows_of([left, right])

    def edge(at):
        cut = slice(at, at + 1)
        fields = (disp[0, cut], disp[1, cut], energy[cut] * mass[cut])
        return rows_of([f[:, h : h + 128] for f in fields for h in (0, 128)] + [left, right])

    tail = jnp.concatenate([coords, edge(ROWS - 1)], axis=0).astype(bf16)
    head = jnp.concatenate([coords, edge(0)], axis=0).astype(bf16)
    for d in range(NGX):
        out[d] = head
    out[lax.rem(gx + 1, NGX)] = tail


def zone_forces(ids, recv, sides, disp, energy, mass, field, force):
    _, gx, gy = place(ids)
    above = recv[lax.rem(gx + NGX - 1, NGX)].astype(f32)[8:16]
    below = recv[lax.rem(gx + 1, NGX)].astype(f32)[8:16]
    row8, lane8 = iota((8, 128), 0), iota((8, 128), 1)
    line, lane = iota((ROWS, 128), 0), iota((ROWS, 128), 1)
    lane1 = iota((1, 128), 1)

    def corner(rows, k, at):
        return jnp.sum(jnp.where(lane1 == at, rows[k : k + 1], 0.0), axis=1, keepdims=True)

    for c in range(3):
        own = energy[...] * mass[...] if c == 2 else disp[c]
        field[c, 0:ROWS, 0:COLS] = own
        for h in range(2):
            k = 2 * c + h
            field[c, ROWS : ROWS + 8, 128 * h : 128 * h + 128] = jnp.where(
                row8 == 0, below[k : k + 1], jnp.where(row8 == 7, above[k : k + 1], 0.0)
            )
        cols = [
            jnp.sum(jnp.where(lane == line + 32 * c, sides[k : k + 1], 0.0), axis=1, keepdims=True)
            for k in range(2)
        ]
        field[c, 0:ROWS, COLS : COLS + 128] = jnp.where(
            lane == 0, cols[1], jnp.where(lane == 127, cols[0], 0.0)
        )
        first, last = 32 * c, 32 * c + 31
        low = jnp.where(
            lane8 == 0, corner(below, 7, first), jnp.where(lane8 == 127, corner(below, 6, first), 0.0)
        )
        high = jnp.where(
            lane8 == 0, corner(above, 7, last), jnp.where(lane8 == 127, corner(above, 6, last), 0.0)
        )
        field[c, ROWS : ROWS + 8, COLS : COLS + 128] = jnp.where(
            row8 == 0, low, jnp.where(row8 == 7, high, 0.0)
        )

    height, width = ROWS + 8, COLS + 128

    def next_row(v):
        return pltpu.roll(v, height - 1, 0)

    def next_col(v):
        return pltpu.roll(v, width - 1, 1)

    def prev_row(v):
        return pltpu.roll(v, 1, 0)

    def prev_col(v):
        return pltpu.roll(v, 1, 1)

    first, second = [], []
    for c in range(2):
        a = field[c]
        b = next_row(a)
        first.append(next_col(b) - a + 1.0)
        second.append(next_col(a) - b + (-1.0 if c == 0 else 1.0))
    at_row, at_col = iota((height, width), 0), iota((height, width), 1)
    zone_row = jnp.where(at_row == height - 1, -1, at_row)
    zone_col = jnp.where(at_col == width - 1, -1, at_col)
    in_row, in_col = gx * ROWS + zone_row, gy * COLS + zone_col
    live = (
        (zone_row < ROWS)
        & (zone_col < COLS)
        & (in_row >= 0)
        & (in_row < TOTAL_ROWS - 1)
        & (in_col >= 0)
        & (in_col < TOTAL_COLS - 1)
    )
    area = jnp.where(live, 0.5 * (first[0] * second[1] - second[0] * first[1]), 1.0)
    press = jnp.where(live, 0.2 * field[2] / area, 0.0)
    on_a = (-press * second[1], press * second[0])
    on_b = (press * first[1], -press * first[0])
    for c in range(2):
        total = (on_a[c] - prev_col(on_b[c])) + prev_row(on_b[c] - prev_col(on_a[c]))
        force[c] = total[0:ROWS, 0:COLS]
    scale = jnp.where(
        live[0:ROWS, 0:COLS], jnp.sqrt(area[0:ROWS, 0:COLS]) / jnp.sqrt(0.56 * energy[...]), 1e30
    )
    return jnp.min(scale, axis=0, keepdims=True)


def contact_terms(slave_x, slave_y, start_x, start_y, end_x, end_y, side, live):
    rel_x = slave_x - start_x + 0.5
    rel_y = slave_y - start_y
    along_x = 1.0 + end_x - start_x
    along_y = end_y - start_y
    along_sq = along_x * along_x + along_y * along_y
    length = jnp.sqrt(along_sq)
    fraction = (rel_x * along_x + rel_y * along_y) / along_sq
    normal_x = -along_y / length
    normal_y = along_x / length
    gap_size = normal_x * rel_x + normal_y * rel_y
    sign = 1.0 - 2.0 * side.astype(f32)
    depth = -sign * gap_size / GAP_SCALE
    soft = jnp.maximum(depth, 0.0) + jnp.log1p(jnp.exp(-jnp.abs(depth)))
    magnitude = jnp.where(live, STIFFNESS * GAP_SCALE * soft, 0.0)
    return magnitude * sign * normal_x, magnitude * sign * normal_y, magnitude, fraction


def high_low(v):
    high = v.astype(bf16).astype(f32)
    return high, v - high


def one_hot(count, index):
    at = lax.broadcasted_iota(jnp.int32, (count, index.shape[1]), 0).astype(f32).astype(bf16)
    return jnp.where(at == index.astype(f32).astype(bf16), jnp.ones((), bf16), jnp.zeros((), bf16))


def node_place(node):
    row = ((node >> 7) & 1) * 32 + (node >> 8)
    return one_hot(128, node & 127), iota((64, PAIRS), 0) == row


def slave_places(disp, pair_node, nodes):
    for c in range(2):
        for h in range(2):
            rest = disp[c, :, 128 * h : 128 * h + 128]
            for k in range(3):
                high, low = high_low(rest)
                at = 128 * k + 64 * c + 32 * h
                nodes[at : at + 32] = high.astype(bf16)
                rest = low
    lanes, mask = node_place(pair_node[...])
    seen = jnp.dot(nodes[...], lanes, preferred_element_type=f32)
    seen = (seen[256:384] + seen[128:256]) + seen[0:128]
    found = [
        jnp.sum(jnp.where(mask, seen[64 * c : 64 * c + 64], 0.0), axis=0, keepdims=True)
        for c in range(2)
    ]
    return found, lanes, mask


def contact_kernel(
    ids,
    count,
    recv,
    sides,
    disp,
    energy,
    mass,
    pair_node,
    pair_segment,
    pair_side,
    out,
    force,
    field,
    coords,
    nodes,
    picks,
):
    slave, node_lanes, node_mask = slave_places(disp, pair_node, nodes)
    row8 = iota((8, 128), 0)
    for i in range(NGX // 4):
        left, right = [], []
        for s in (4 * i, 4 * i + 2):
            even, odd = recv[s, 0:8].astype(f32), recv[s + 1, 0:8].astype(f32)
            left.append(jnp.where(row8 < 4, even, pltpu.roll(odd, 4, 0)))
            right.append(jnp.where(row8 < 4, pltpu.roll(even, 4, 0), odd))
        coords[16 * i : 16 * i + 16, 0:128] = jnp.concatenate(left, axis=0).astype(bf16)
        coords[16 * i : 16 * i + 16, 128:256] = jnp.concatenate(right, axis=0).astype(bf16)

    segment = pair_segment[...]
    ends = jnp.concatenate([segment, segment + 1], axis=1)
    lanes = one_hot(256, ends & 255)
    piece, line = ends >> 9, (ends >> 8) & 1
    looked = jnp.dot(coords[...], lanes, preferred_element_type=f32)
    found = jnp.zeros((8, 2 * PAIRS), f32)
    for s in range(NGX // 2):
        found = found + jnp.where((piece >> 1) == s, looked[8 * s : 8 * s + 8], 0.0)
    row = iota((8, 2 * PAIRS), 0)
    at = (piece & 1) * 4 + line
    end_x = jnp.sum(jnp.where(row == at, found, 0.0), axis=0, keepdims=True)
    end_y = jnp.sum(jnp.where(row == at + 2, found, 0.0), axis=0, keepdims=True)

    live = iota((1, PAIRS), 1).astype(f32) < count[0:1, 0:1]
    push_x, push_y, magnitude, fraction = contact_terms(
        slave[0],
        slave[1],
        end_x[:, :PAIRS],
        end_y[:, :PAIRS],
        end_x[:, PAIRS:],
        end_y[:, PAIRS:],
        pair_side[...],
        live,
    )
    share = jnp.concatenate([1.0 - fraction, fraction], axis=1)
    terms = [share * jnp.concatenate([v, v], axis=1) for v in (-push_x, -push_y, magnitude)]
    stacked = jnp.where(row < 2, terms[0], jnp.where(row < 4, terms[1], terms[2]))
    stacked = jnp.where((row < 6) & ((row & 1) == line), stacked, 0.0)
    high, low = high_low(stacked)
    high = jnp.concatenate([high, high], axis=0).astype(bf16)
    low = jnp.concatenate([low, low], axis=0).astype(bf16)
    half = iota((16, 2 * PAIRS), 0) >> 3
    offset = (piece - half).astype(f32).astype(bf16)
    nothing = jnp.zeros((), bf16)
    for s in range(NGX // 2):
        mine = offset == jnp.asarray(2 * s, bf16)
        picks[16 * s : 16 * s + 16] = jnp.where(mine, high, nothing)
        picks[256 + 16 * s : 272 + 16 * s] = jnp.where(mine, low, nothing)
    contract = (((1,), (1,)), ((), ()))
    part = lax.dot_general(picks[...], lanes, contract, preferred_element_type=f32)
    reaction = part[0:256] + part[256:512]

    rows = [jnp.where(node_mask, half, 0.0) for v in (push_x, push_y) for half in high_low(v)]
    rows = jnp.concatenate([rows[0], rows[2], rows[1], rows[3]], axis=0).astype(bf16)
    part = lax.dot_general(rows, node_lanes, contract, preferred_element_type=f32)
    pushed = part[0:128] + part[128:256]

    least = zone_forces(ids, recv, sides, disp, energy, mass, field, force)
    for c in range(2):
        for h in range(2):
            at = 64 * c + 32 * h
            force[c, :, 128 * h : 128 * h + 128] += pushed[at : at + 32]
    row = iota((8, 256), 0)
    for s in range(NGX):
        out[s] = jnp.where(row == 6, least, reaction[8 * s : 8 * s + 8])


def sum_kernel(recv, chunk, out):
    total = recv[0]
    least = recv[0]
    for s in range(1, NGX):
        part = recv[s]
        total = total + part
        least = jnp.minimum(least, part)
    least = jnp.min(least[6:7], axis=1, keepdims=True)
    lane = iota((1, 128), 1)
    for z in range(NGY):
        rows = total[:, 128 * ((z % 8) // 4) : 128 * ((z % 8) // 4) + 128]
        line = jnp.broadcast_to(least, (1, 128))
        old = jnp.zeros((1, 128), f32)
        for c in range(3):
            shift = 32 * ((c - z) % 4)
            mine = (lane >= 32 * c) & (lane < 32 * c + 32)
            row = rows[2 * c + z // 8 : 2 * c + z // 8 + 1]
            line = jnp.where(mine, pltpu.roll(row, shift, 1) if shift else row, line)
            if c < 2:
                row = chunk[z // 4, 2 + c : 3 + c].astype(f32)
                old = jnp.where(mine, pltpu.roll(row, shift, 1) if shift else row, old)
        out[z, 0:1] = line
        out[z, 1:2] = old


def step_kernel(recv, force, vel, disp, mass, new_vel, new_disp, master):
    total = recv[0]
    least = recv[0]
    for z in range(1, NGY):
        part = recv[z]
        total = total + part
        least = jnp.minimum(least, part)
    lane = iota((1, 128), 1)
    least = jnp.where(lane >= 96, least[0:1], 1e30)
    step = 0.3 * jnp.min(least, axis=1, keepdims=True)
    for c in range(2):
        vel_c = vel[c] + step * force[c] / mass[...]
        new_vel[c] = vel_c
        new_disp[c] = disp[c] + step * vel_c
    moved = total[1:2] + step * total[0:1]
    for c in range(3):
        master[c : c + 1, :] = moved[:, 32 * c : 32 * c + 32]


def call(kernel, out, ins, scratch=(), flops=1_000_000):
    return pl.pallas_call(
        kernel,
        out_shape=[jax.ShapeDtypeStruct(s, d) for s, d in out],
        in_specs=[SMEM if i == "s" else VMEM for i in ins],
        out_specs=[VMEM] * len(out),
        scratch_shapes=[pltpu.VMEM(s, d) for s, d in scratch],
        compiler_params=pltpu.CompilerParams(vmem_limit_bytes=16 << 20),
        cost_estimate=pl.CostEstimate(flops=flops, bytes_accessed=1 << 20, transcendentals=0),
    )


def exchange(value, axes):
    return lax.all_to_all(value, axes, 0, 0, tiled=True)


def owner_piece(exchange, master_block, owner, count):
    tiles = master_block[0].reshape(4, NGX, 4, 128).transpose(1, 2, 0, 3)
    out = [((4, 4, 128), bf16), ((8, 128), f32)]

    def send(tiles, owner, count):
        return tuple(call(pick_kernel, out, "ssv")(owner, count, exchange(tiles, GX)))

    def idle(tiles, owner, count):
        return tuple(call(idle_kernel, out, "s")(count))

    mine = lax.axis_index("gy") == (owner[0] & (NGY - 1))
    return lax.cond(mine, send, idle, tiles, owner, count)


def stages(
    exchange,
    node_disp,
    node_vel,
    node_mass,
    zone_mass,
    zone_energy,
    master_block,
    owner,
    pair_node,
    pair_segment,
    pair_side,
    pair_count,
):
    fields = (node_disp, zone_energy, zone_mass)
    chunk, count = owner_piece(exchange, master_block, owner, pair_count)
    (sent,) = call(spread_kernel, [((NGY, 3, 4, 128), bf16)], "vvvv")(chunk, *fields)
    sent = exchange(sent, "gy")
    sent, sides = call(gather_kernel, [((NGX, 16, 128), bf16), ((8, 128), f32)], "svvvv")(
        owner, sent, *fields
    )
    sent = exchange(sent, GX)
    sent, force = call(
        contact_kernel,
        [((NGX, 8, 256), f32), ((2, ROWS, COLS), f32)],
        "svvvvvvvvv",
        [
            ((3, ROWS + 8, COLS + 128), f32),
            ((128, 256), bf16),
            ((384, 128), bf16),
            ((512, 2 * PAIRS), bf16),
        ],
    )(owner, count, sent, sides, *fields, pair_node, pair_segment, pair_side)
    sent = exchange(sent, GX)
    (sent,) = call(sum_kernel, [((NGY, 2, 128), f32)], "vv")(sent, chunk)
    sent = exchange(sent, "gy")
    return tuple(
        call(
            step_kernel,
            [((2, ROWS, COLS), f32), ((2, ROWS, COLS), f32), ((3, 32), f32)],
            "vvvvv",
        )(sent, force, node_vel, node_disp, node_mass)
    )


def shards(*args):
    return stages(exchange, *args)


def solution(mesh):
    split = Mesh(mesh.devices.reshape(4, 4, 2, mesh.shape["gy"]), ("gx_0", "gx_1", "gx_2", "gy"))
    in_specs = (
        P(None, GX, "gy"),
        P(None, GX, "gy"),
        P(GX, "gy"),
        P(GX, "gy"),
        P(GX, "gy"),
        P(GX_GY, None, None),
        P(),
        P(GX_GY, None),
        P(GX_GY, None),
        P(GX_GY, None),
        P(GX_GY),
    )
    out_specs = (P(None, GX, "gy"), P(None, GX, "gy"), P(None, GX_GY))
    return jax.shard_map(
        shards, mesh=split, in_specs=in_specs, out_specs=out_specs, check_vma=False
    )
```

```python
import jax
import jax.numpy as jnp
from jax import lax
from jax.experimental import pallas as pl
from jax.experimental.pallas import tpu as pltpu
from jax.sharding import Mesh
from jax.sharding import PartitionSpec as P

GX = ("gx_0", "gx_1", "gx_2")
GX_GY = ("gx_0", "gx_1", "gx_2", "gy")
NGX = 32
NGY = 16
ROWS = 32
COLS = 256
PAIRS = 1024
TOTAL_ROWS = NGX * ROWS
TOTAL_COLS = NGY * COLS
STIFFNESS = 10.0
GAP_SCALE = 0.05

f32 = jnp.float32
bf16 = jnp.bfloat16
VMEM = pl.BlockSpec(memory_space=pltpu.VMEM)
SMEM = pl.BlockSpec(memory_space=pltpu.SMEM)


def place(ids):
    return ids[0], lax.axis_index(GX), lax.axis_index("gy")


def iota(shape, dim):
    return lax.broadcasted_iota(jnp.int32, shape, dim)


def rows_of(pieces):
    row = iota((8, 128), 0)
    tile = jnp.zeros((8, 128), f32)
    for k, piece in enumerate(pieces):
        tile = jnp.where(row == k, piece, tile)
    return tile


def column_row(columns):
    line, lane = iota((ROWS, 128), 0), iota((ROWS, 128), 1)
    out = jnp.zeros((ROWS, 128), f32)
    for c, column in enumerate(columns):
        out = jnp.where(lane == line + 32 * c, column, out)
    return jnp.sum(out, axis=0, keepdims=True)


def count_tile(count):
    return jnp.full((8, 128), count[0].astype(f32))


def tile_kernel(owner, count, tile, at):
    tile[...] = count_tile(count)
    at[...] = jnp.full((8, 128), owner[0] // NGY)


def pick_kernel(at, recv, chunk):
    picked = jnp.zeros((4, 4, 128), f32)
    for s in range(NGX):
        picked = jnp.where((at[0:4] == s)[None], recv[s].astype(f32), picked)
    chunk[...] = picked.astype(bf16)


def idle_kernel(count, chunk, tile):
    chunk[...] = jnp.zeros((4, 4, 128), bf16)
    tile[...] = count_tile(count)


def spread_kernel(chunk, disp, energy, mass, out):
    for h in range(2):
        rows = [chunk[2 * r + h, c : c + 1].astype(f32) for c in range(2) for r in range(2)]
        coords = rows_of(rows)[0:4].astype(bf16)
        for z in range(NGY):
            out[z, h] = coords

    def edge(at):
        cut = slice(at, at + 1)
        columns = [disp[0, :, cut], disp[1, :, cut], energy[:, cut] * mass[:, cut]]
        return rows_of([column_row(columns)])[0:4].astype(bf16)

    head, tail = edge(0), edge(COLS - 1)
    for z in range(NGY):
        out[z, 2] = head
    out[lax.rem(lax.axis_index("gy") + 1, NGY), 2] = tail


def gather_kernel(ids, recv, disp, energy, mass, out, sides):
    owner, gx, gy = place(ids)
    picked = recv[lax.rem(owner, NGY)].astype(f32)
    left = recv[lax.rem(gy + NGY - 1, NGY), 2].astype(f32)[0:1]
    right = recv[lax.rem(gy + 1, NGY), 2].astype(f32)[0:1]
    coords = jnp.concatenate([picked[0], picked[1]], axis=0)
    sides[...] = rows_of([left, right])

    def edge(at):
        cut = slice(at, at + 1)
        fields = (disp[0, cut], disp[1, cut], energy[cut] * mass[cut])
        return rows_of([f[:, h : h + 128] for f in fields for h in (0, 128)] + [left, right])

    tail = jnp.concatenate([coords, edge(ROWS - 1)], axis=0).astype(bf16)
    head = jnp.concatenate([coords, edge(0)], axis=0).astype(bf16)
    for d in range(NGX):
        out[d] = head
    out[lax.rem(gx + 1, NGX)] = tail


def zone_forces(ids, recv, sides, disp, energy, mass, field, force):
    _, gx, gy = place(ids)
    above = recv[lax.rem(gx + NGX - 1, NGX)].astype(f32)[8:16]
    below = recv[lax.rem(gx + 1, NGX)].astype(f32)[8:16]
    row8, lane8 = iota((8, 128), 0), iota((8, 128), 1)
    line, lane = iota((ROWS, 128), 0), iota((ROWS, 128), 1)
    lane1 = iota((1, 128), 1)

    def corner(rows, k, at):
        return jnp.sum(jnp.where(lane1 == at, rows[k : k + 1], 0.0), axis=1, keepdims=True)

    for c in range(3):
        own = energy[...] * mass[...] if c == 2 else disp[c]
        field[c, 0:ROWS, 0:COLS] = own
        for h in range(2):
            k = 2 * c + h
            field[c, ROWS : ROWS + 8, 128 * h : 128 * h + 128] = jnp.where(
                row8 == 0, below[k : k + 1], jnp.where(row8 == 7, above[k : k + 1], 0.0)
            )
        cols = [
            jnp.sum(jnp.where(lane == line + 32 * c, sides[k : k + 1], 0.0), axis=1, keepdims=True)
            for k in range(2)
        ]
        field[c, 0:ROWS, COLS : COLS + 128] = jnp.where(
            lane == 0, cols[1], jnp.where(lane == 127, cols[0], 0.0)
        )
        first, last = 32 * c, 32 * c + 31
        low = jnp.where(
            lane8 == 0, corner(below, 7, first), jnp.where(lane8 == 127, corner(below, 6, first), 0.0)
        )
        high = jnp.where(
            lane8 == 0, corner(above, 7, last), jnp.where(lane8 == 127, corner(above, 6, last), 0.0)
        )
        field[c, ROWS : ROWS + 8, COLS : COLS + 128] = jnp.where(
            row8 == 0, low, jnp.where(row8 == 7, high, 0.0)
        )

    height, width = ROWS + 8, COLS + 128

    def next_row(v):
        return pltpu.roll(v, height - 1, 0)

    def next_col(v):
        return pltpu.roll(v, width - 1, 1)

    def prev_row(v):
        return pltpu.roll(v, 1, 0)

    def prev_col(v):
        return pltpu.roll(v, 1, 1)

    first, second = [], []
    for c in range(2):
        a = field[c]
        b = next_row(a)
        first.append(next_col(b) - a + 1.0)
        second.append(next_col(a) - b + (-1.0 if c == 0 else 1.0))
    at_row, at_col = iota((height, width), 0), iota((height, width), 1)
    zone_row = jnp.where(at_row == height - 1, -1, at_row)
    zone_col = jnp.where(at_col == width - 1, -1, at_col)
    in_row, in_col = gx * ROWS + zone_row, gy * COLS + zone_col
    live = (
        (zone_row < ROWS)
        & (zone_col < COLS)
        & (in_row >= 0)
        & (in_row < TOTAL_ROWS - 1)
        & (in_col >= 0)
        & (in_col < TOTAL_COLS - 1)
    )
    area = jnp.where(live, 0.5 * (first[0] * second[1] - second[0] * first[1]), 1.0)
    press = jnp.where(live, 0.2 * field[2] / area, 0.0)
    on_a = (-press * second[1], press * second[0])
    on_b = (press * first[1], -press * first[0])
    for c in range(2):
        total = (on_a[c] - prev_col(on_b[c])) + prev_row(on_b[c] - prev_col(on_a[c]))
        force[c] = total[0:ROWS, 0:COLS]
    scale = jnp.where(
        live[0:ROWS, 0:COLS], jnp.sqrt(area[0:ROWS, 0:COLS]) / jnp.sqrt(0.56 * energy[...]), 1e30
    )
    return jnp.min(scale, axis=0, keepdims=True)


def contact_terms(slave_x, slave_y, start_x, start_y, end_x, end_y, side, live):
    rel_x = slave_x - start_x + 0.5
    rel_y = slave_y - start_y
    along_x = 1.0 + end_x - start_x
    along_y = end_y - start_y
    along_sq = along_x * along_x + along_y * along_y
    length = jnp.sqrt(along_sq)
    fraction = (rel_x * along_x + rel_y * along_y) / along_sq
    normal_x = -along_y / length
    normal_y = along_x / length
    gap_size = normal_x * rel_x + normal_y * rel_y
    sign = 1.0 - 2.0 * side.astype(f32)
    depth = -sign * gap_size / GAP_SCALE
    soft = jnp.maximum(depth, 0.0) + jnp.log1p(jnp.exp(-jnp.abs(depth)))
    magnitude = jnp.where(live, STIFFNESS * GAP_SCALE * soft, 0.0)
    return magnitude * sign * normal_x, magnitude * sign * normal_y, magnitude, fraction


def high_low(v):
    high = v.astype(bf16).astype(f32)
    return high, v - high


def one_hot(count, index):
    at = lax.broadcasted_iota(jnp.int32, (count, index.shape[1]), 0).astype(f32).astype(bf16)
    return jnp.where(at == index.astype(f32).astype(bf16), jnp.ones((), bf16), jnp.zeros((), bf16))


def node_place(node):
    row = ((node >> 7) & 1) * 32 + (node >> 8)
    return one_hot(128, node & 127), iota((64, PAIRS), 0) == row


def slave_places(disp, pair_node, nodes):
    for c in range(2):
        for h in range(2):
            rest = disp[c, :, 128 * h : 128 * h + 128]
            for k in range(3):
                high, low = high_low(rest)
                at = 128 * k + 64 * c + 32 * h
                nodes[at : at + 32] = high.astype(bf16)
                rest = low
    lanes, mask = node_place(pair_node[...])
    seen = jnp.dot(nodes[...], lanes, preferred_element_type=f32)
    seen = (seen[256:384] + seen[128:256]) + seen[0:128]
    found = [
        jnp.sum(jnp.where(mask, seen[64 * c : 64 * c + 64], 0.0), axis=0, keepdims=True)
        for c in range(2)
    ]
    return found, lanes, mask


def contact_kernel(
    ids,
    count,
    recv,
    sides,
    disp,
    energy,
    mass,
    pair_node,
    pair_segment,
    pair_side,
    out,
    force,
    field,
    coords,
    nodes,
    picks,
):
    slave, node_lanes, node_mask = slave_places(disp, pair_node, nodes)
    row8 = iota((8, 128), 0)
    for i in range(NGX // 4):
        left, right = [], []
        for s in (4 * i, 4 * i + 2):
            even, odd = recv[s, 0:8].astype(f32), recv[s + 1, 0:8].astype(f32)
            left.append(jnp.where(row8 < 4, even, pltpu.roll(odd, 4, 0)))
            right.append(jnp.where(row8 < 4, pltpu.roll(even, 4, 0), odd))
        coords[16 * i : 16 * i + 16, 0:128] = jnp.concatenate(left, axis=0).astype(bf16)
        coords[16 * i : 16 * i + 16, 128:256] = jnp.concatenate(right, axis=0).astype(bf16)

    segment = pair_segment[...]
    ends = jnp.concatenate([segment, segment + 1], axis=1)
    lanes = one_hot(256, ends & 255)
    piece, line = ends >> 9, (ends >> 8) & 1
    looked = jnp.dot(coords[...], lanes, preferred_element_type=f32)
    found = jnp.zeros((8, 2 * PAIRS), f32)
    for s in range(NGX // 2):
        found = found + jnp.where((piece >> 1) == s, looked[8 * s : 8 * s + 8], 0.0)
    row = iota((8, 2 * PAIRS), 0)
    at = (piece & 1) * 4 + line
    end_x = jnp.sum(jnp.where(row == at, found, 0.0), axis=0, keepdims=True)
    end_y = jnp.sum(jnp.where(row == at + 2, found, 0.0), axis=0, keepdims=True)

    live = iota((1, PAIRS), 1).astype(f32) < count[0:1, 0:1]
    push_x, push_y, magnitude, fraction = contact_terms(
        slave[0],
        slave[1],
        end_x[:, :PAIRS],
        end_y[:, :PAIRS],
        end_x[:, PAIRS:],
        end_y[:, PAIRS:],
        pair_side[...],
        live,
    )
    share = jnp.concatenate([1.0 - fraction, fraction], axis=1)
    terms = [share * jnp.concatenate([v, v], axis=1) for v in (-push_x, -push_y, magnitude)]
    stacked = jnp.where(row < 2, terms[0], jnp.where(row < 4, terms[1], terms[2]))
    stacked = jnp.where((row < 6) & ((row & 1) == line), stacked, 0.0)
    high, low = high_low(stacked)
    high = jnp.concatenate([high, high], axis=0).astype(bf16)
    low = jnp.concatenate([low, low], axis=0).astype(bf16)
    half = iota((16, 2 * PAIRS), 0) >> 3
    offset = (piece - half).astype(f32).astype(bf16)
    nothing = jnp.zeros((), bf16)
    for s in range(NGX // 2):
        mine = offset == jnp.asarray(2 * s, bf16)
        picks[16 * s : 16 * s + 16] = jnp.where(mine, high, nothing)
        picks[256 + 16 * s : 272 + 16 * s] = jnp.where(mine, low, nothing)
    contract = (((1,), (1,)), ((), ()))
    part = lax.dot_general(picks[...], lanes, contract, preferred_element_type=f32)
    reaction = part[0:256] + part[256:512]

    rows = [jnp.where(node_mask, half, 0.0) for v in (push_x, push_y) for half in high_low(v)]
    rows = jnp.concatenate([rows[0], rows[2], rows[1], rows[3]], axis=0).astype(bf16)
    part = lax.dot_general(rows, node_lanes, contract, preferred_element_type=f32)
    pushed = part[0:128] + part[128:256]

    least = zone_forces(ids, recv, sides, disp, energy, mass, field, force)
    for c in range(2):
        for h in range(2):
            at = 64 * c + 32 * h
            force[c, :, 128 * h : 128 * h + 128] += pushed[at : at + 32]
    row = iota((8, 256), 0)
    for s in range(NGX):
        out[s] = jnp.where(row == 6, least, reaction[8 * s : 8 * s + 8])


def sum_kernel(recv, chunk, out):
    total = recv[0]
    least = recv[0]
    for s in range(1, NGX):
        part = recv[s]
        total = total + part
        least = jnp.minimum(least, part)
    least = jnp.min(least[6:7], axis=1, keepdims=True)
    lane = iota((1, 128), 1)
    for z in range(NGY):
        rows = total[:, 128 * ((z % 8) // 4) : 128 * ((z % 8) // 4) + 128]
        line = jnp.broadcast_to(least, (1, 128))
        old = jnp.zeros((1, 128), f32)
        for c in range(3):
            shift = 32 * ((c - z) % 4)
            mine = (lane >= 32 * c) & (lane < 32 * c + 32)
            row = rows[2 * c + z // 8 : 2 * c + z // 8 + 1]
            line = jnp.where(mine, pltpu.roll(row, shift, 1) if shift else row, line)
            if c < 2:
                row = chunk[z // 4, 2 + c : 3 + c].astype(f32)
                old = jnp.where(mine, pltpu.roll(row, shift, 1) if shift else row, old)
        out[z, 0:1] = line
        out[z, 1:2] = old


def step_kernel(recv, force, vel, disp, mass, new_vel, new_disp, master):
    total = recv[0]
    least = recv[0]
    for z in range(1, NGY):
        part = recv[z]
        total = total + part
        least = jnp.minimum(least, part)
    lane = iota((1, 128), 1)
    least = jnp.where(lane >= 96, least[0:1], 1e30)
    step = 0.3 * jnp.min(least, axis=1, keepdims=True)
    for c in range(2):
        vel_c = vel[c] + step * force[c] / mass[...]
        new_vel[c] = vel_c
        new_disp[c] = disp[c] + step * vel_c
    moved = total[1:2] + step * total[0:1]
    for c in range(3):
        master[c : c + 1, :] = moved[:, 32 * c : 32 * c + 32]


def call(kernel, out, ins, scratch=(), flops=1_000_000):
    return pl.pallas_call(
        kernel,
        out_shape=[jax.ShapeDtypeStruct(s, d) for s, d in out],
        in_specs=[SMEM if i == "s" else VMEM for i in ins],
        out_specs=[VMEM] * len(out),
        scratch_shapes=[pltpu.VMEM(s, d) for s, d in scratch],
        compiler_params=pltpu.CompilerParams(vmem_limit_bytes=16 << 20),
        cost_estimate=pl.CostEstimate(flops=flops, bytes_accessed=1 << 20, transcendentals=0),
    )


def exchange(value, axes):
    return lax.all_to_all(value, axes, 0, 0, tiled=True)


def owner_piece(exchange, master_block, owner, count):
    tiles = master_block[0].reshape(4, NGX, 4, 128).transpose(1, 2, 0, 3)
    out = [((4, 4, 128), bf16), ((8, 128), f32)]

    def send(tiles, owner, count):
        recv = exchange(tiles, GX)
        tile, at = call(tile_kernel, [out[1], ((8, 128), jnp.int32)], "ss", flops=100_000_000)(owner, count)
        return call(pick_kernel, out[:1], "vv")(at, recv)[0], tile

    def idle(tiles, owner, count):
        return tuple(call(idle_kernel, out, "s")(count))

    mine = lax.axis_index("gy") == (owner[0] & (NGY - 1))
    return lax.cond(mine, send, idle, tiles, owner, count)


def stages(
    exchange,
    node_disp,
    node_vel,
    node_mass,
    zone_mass,
    zone_energy,
    master_block,
    owner,
    pair_node,
    pair_segment,
    pair_side,
    pair_count,
):
    fields = (node_disp, zone_energy, zone_mass)
    chunk, count = owner_piece(exchange, master_block, owner, pair_count)
    (sent,) = call(spread_kernel, [((NGY, 3, 4, 128), bf16)], "vvvv")(chunk, *fields)
    sent = exchange(sent, "gy")
    sent, sides = call(gather_kernel, [((NGX, 16, 128), bf16), ((8, 128), f32)], "svvvv")(
        owner, sent, *fields
    )
    sent = exchange(sent, GX)
    sent, force = call(
        contact_kernel,
        [((NGX, 8, 256), f32), ((2, ROWS, COLS), f32)],
        "svvvvvvvvv",
        [
            ((3, ROWS + 8, COLS + 128), f32),
            ((128, 256), bf16),
            ((384, 128), bf16),
            ((512, 2 * PAIRS), bf16),
        ],
    )(owner, count, sent, sides, *fields, pair_node, pair_segment, pair_side)
    sent = exchange(sent, GX)
    (sent,) = call(sum_kernel, [((NGY, 2, 128), f32)], "vv")(sent, chunk)
    sent = exchange(sent, "gy")
    return tuple(
        call(
            step_kernel,
            [((2, ROWS, COLS), f32), ((2, ROWS, COLS), f32), ((3, 32), f32)],
            "vvvvv",
        )(sent, force, node_vel, node_disp, node_mass)
    )


def shards(*args):
    return stages(exchange, *args)


def solution(mesh):
    split = Mesh(mesh.devices.reshape(4, 4, 2, mesh.shape["gy"]), ("gx_0", "gx_1", "gx_2", "gy"))
    in_specs = (
        P(None, GX, "gy"),
        P(None, GX, "gy"),
        P(GX, "gy"),
        P(GX, "gy"),
        P(GX, "gy"),
        P(GX_GY, None, None),
        P(),
        P(GX_GY, None),
        P(GX_GY, None),
        P(GX_GY, None),
        P(GX_GY),
    )
    out_specs = (P(None, GX, "gy"), P(None, GX, "gy"), P(None, GX_GY))
    return jax.shard_map(
        shards, mesh=split, in_specs=in_specs, out_specs=out_specs, check_vma=False
    )
```

```python
import jax
import jax.numpy as jnp
from jax import lax
from jax.experimental import pallas as pl
from jax.experimental.pallas import tpu as pltpu
from jax.sharding import Mesh
from jax.sharding import PartitionSpec as P

GX = ("gx_0", "gx_1", "gx_2")
GX_GY = ("gx_0", "gx_1", "gx_2", "gy")
NGX = 32
NGY = 16
ROWS = 32
COLS = 256
PAIRS = 1024
TOTAL_ROWS = NGX * ROWS
TOTAL_COLS = NGY * COLS
STIFFNESS = 10.0
GAP_SCALE = 0.05

f32 = jnp.float32
bf16 = jnp.bfloat16
VMEM = pl.BlockSpec(memory_space=pltpu.VMEM)
SMEM = pl.BlockSpec(memory_space=pltpu.SMEM)


def place(ids):
    return ids[0], lax.axis_index(GX), lax.axis_index("gy")


def iota(shape, dim):
    return lax.broadcasted_iota(jnp.int32, shape, dim)


def rows_of(pieces):
    row = iota((8, 128), 0)
    tile = jnp.zeros((8, 128), f32)
    for k, piece in enumerate(pieces):
        tile = jnp.where(row == k, piece, tile)
    return tile


def column_row(columns):
    line, lane = iota((ROWS, 128), 0), iota((ROWS, 128), 1)
    out = jnp.zeros((ROWS, 128), f32)
    for c, column in enumerate(columns):
        out = jnp.where(lane == line + 32 * c, column, out)
    return jnp.sum(out, axis=0, keepdims=True)


def count_tile(count):
    return jnp.full((8, 128), count[0].astype(f32))


def tile_kernel(owner, count, tile, at):
    tile[...] = count_tile(count)
    at[...] = jnp.full((8, 128), owner[0] // NGY)


def pick_kernel(at, recv, chunk):
    picked = jnp.zeros((4, 4, 128), f32)
    for s in range(NGX):
        picked = jnp.where((at[0:4] == s)[None], recv[s].astype(f32), picked)
    chunk[...] = picked.astype(bf16)


def idle_kernel(count, chunk, tile):
    chunk[...] = jnp.zeros((4, 4, 128), bf16)
    tile[...] = count_tile(count)


def spread_kernel(chunk, disp, energy, mass, out):
    for h in range(2):
        rows = [chunk[2 * r + h, c : c + 1].astype(f32) for c in range(2) for r in range(2)]
        coords = rows_of(rows)[0:4].astype(bf16)
        for z in range(NGY):
            out[z, h] = coords

    def edge(at):
        cut = slice(at, at + 1)
        columns = [disp[0, :, cut], disp[1, :, cut], energy[:, cut] * mass[:, cut]]
        return rows_of([column_row(columns)])[0:4].astype(bf16)

    head, tail = edge(0), edge(COLS - 1)
    for z in range(NGY):
        out[z, 2] = head
    out[lax.rem(lax.axis_index("gy") + 1, NGY), 2] = tail


def gather_kernel(ids, recv, disp, energy, mass, out, sides):
    owner, gx, gy = place(ids)
    picked = recv[lax.rem(owner, NGY)].astype(f32)
    left = recv[lax.rem(gy + NGY - 1, NGY), 2].astype(f32)[0:1]
    right = recv[lax.rem(gy + 1, NGY), 2].astype(f32)[0:1]
    coords = jnp.concatenate([picked[0], picked[1]], axis=0)
    sides[...] = rows_of([left, right])

    def edge(at):
        cut = slice(at, at + 1)
        fields = (disp[0, cut], disp[1, cut], energy[cut] * mass[cut])
        return rows_of([f[:, h : h + 128] for f in fields for h in (0, 128)] + [left, right])

    tail = jnp.concatenate([coords, edge(ROWS - 1)], axis=0).astype(bf16)
    head = jnp.concatenate([coords, edge(0)], axis=0).astype(bf16)
    for d in range(NGX):
        out[d] = head
    out[lax.rem(gx + 1, NGX)] = tail


def zone_forces(ids, recv, sides, disp, energy, mass, field, force):
    _, gx, gy = place(ids)
    above = recv[lax.rem(gx + NGX - 1, NGX)].astype(f32)[8:16]
    below = recv[lax.rem(gx + 1, NGX)].astype(f32)[8:16]
    row8, lane8 = iota((8, 128), 0), iota((8, 128), 1)
    line, lane = iota((ROWS, 128), 0), iota((ROWS, 128), 1)
    lane1 = iota((1, 128), 1)

    def corner(rows, k, at):
        return jnp.sum(jnp.where(lane1 == at, rows[k : k + 1], 0.0), axis=1, keepdims=True)

    for c in range(3):
        own = energy[...] * mass[...] if c == 2 else disp[c]
        field[c, 0:ROWS, 0:COLS] = own
        for h in range(2):
            k = 2 * c + h
            field[c, ROWS : ROWS + 8, 128 * h : 128 * h + 128] = jnp.where(
                row8 == 0, below[k : k + 1], jnp.where(row8 == 7, above[k : k + 1], 0.0)
            )
        cols = [
            jnp.sum(jnp.where(lane == line + 32 * c, sides[k : k + 1], 0.0), axis=1, keepdims=True)
            for k in range(2)
        ]
        field[c, 0:ROWS, COLS : COLS + 128] = jnp.where(
            lane == 0, cols[1], jnp.where(lane == 127, cols[0], 0.0)
        )
        first, last = 32 * c, 32 * c + 31
        low = jnp.where(
            lane8 == 0, corner(below, 7, first), jnp.where(lane8 == 127, corner(below, 6, first), 0.0)
        )
        high = jnp.where(
            lane8 == 0, corner(above, 7, last), jnp.where(lane8 == 127, corner(above, 6, last), 0.0)
        )
        field[c, ROWS : ROWS + 8, COLS : COLS + 128] = jnp.where(
            row8 == 0, low, jnp.where(row8 == 7, high, 0.0)
        )

    height, width = ROWS + 8, COLS + 128

    def next_row(v):
        return pltpu.roll(v, height - 1, 0)

    def next_col(v):
        return pltpu.roll(v, width - 1, 1)

    def prev_row(v):
        return pltpu.roll(v, 1, 0)

    def prev_col(v):
        return pltpu.roll(v, 1, 1)

    first, second = [], []
    for c in range(2):
        a = field[c]
        b = next_row(a)
        first.append(next_col(b) - a + 1.0)
        second.append(next_col(a) - b + (-1.0 if c == 0 else 1.0))
    at_row, at_col = iota((height, width), 0), iota((height, width), 1)
    zone_row = jnp.where(at_row == height - 1, -1, at_row)
    zone_col = jnp.where(at_col == width - 1, -1, at_col)
    in_row, in_col = gx * ROWS + zone_row, gy * COLS + zone_col
    live = (
        (zone_row < ROWS)
        & (zone_col < COLS)
        & (in_row >= 0)
        & (in_row < TOTAL_ROWS - 1)
        & (in_col >= 0)
        & (in_col < TOTAL_COLS - 1)
    )
    area = jnp.where(live, 0.5 * (first[0] * second[1] - second[0] * first[1]), 1.0)
    press = jnp.where(live, 0.2 * field[2] / area, 0.0)
    on_a = (-press * second[1], press * second[0])
    on_b = (press * first[1], -press * first[0])
    for c in range(2):
        total = (on_a[c] - prev_col(on_b[c])) + prev_row(on_b[c] - prev_col(on_a[c]))
        force[c] = total[0:ROWS, 0:COLS]
    scale = jnp.where(
        live[0:ROWS, 0:COLS], jnp.sqrt(area[0:ROWS, 0:COLS]) / jnp.sqrt(0.56 * energy[...]), 1e30
    )
    return jnp.min(scale, axis=0, keepdims=True)


def contact_terms(slave_x, slave_y, start_x, start_y, end_x, end_y, side, live):
    rel_x = slave_x - start_x + 0.5
    rel_y = slave_y - start_y
    along_x = 1.0 + end_x - start_x
    along_y = end_y - start_y
    along_sq = along_x * along_x + along_y * along_y
    length = jnp.sqrt(along_sq)
    fraction = (rel_x * along_x + rel_y * along_y) / along_sq
    normal_x = -along_y / length
    normal_y = along_x / length
    gap_size = normal_x * rel_x + normal_y * rel_y
    sign = 1.0 - 2.0 * side.astype(f32)
    depth = -sign * gap_size / GAP_SCALE
    soft = jnp.maximum(depth, 0.0) + jnp.log1p(jnp.exp(-jnp.abs(depth)))
    magnitude = jnp.where(live, STIFFNESS * GAP_SCALE * soft, 0.0)
    return magnitude * sign * normal_x, magnitude * sign * normal_y, magnitude, fraction


def high_low(v):
    high = v.astype(bf16).astype(f32)
    return high, v - high


def one_hot(count, index):
    at = lax.broadcasted_iota(jnp.int32, (count, index.shape[1]), 0).astype(f32).astype(bf16)
    return jnp.where(at == index.astype(f32).astype(bf16), jnp.ones((), bf16), jnp.zeros((), bf16))


def node_place(node):
    row = ((node >> 7) & 1) * 32 + (node >> 8)
    return one_hot(128, node & 127), iota((64, PAIRS), 0) == row


def slave_places(disp, pair_node, nodes):
    for c in range(2):
        for h in range(2):
            rest = disp[c, :, 128 * h : 128 * h + 128]
            for k in range(3):
                high, low = high_low(rest)
                at = 128 * k + 64 * c + 32 * h
                nodes[at : at + 32] = high.astype(bf16)
                rest = low
    lanes, mask = node_place(pair_node[...])
    seen = jnp.dot(nodes[...], lanes, preferred_element_type=f32)
    seen = (seen[256:384] + seen[128:256]) + seen[0:128]
    found = [
        jnp.sum(jnp.where(mask, seen[64 * c : 64 * c + 64], 0.0), axis=0, keepdims=True)
        for c in range(2)
    ]
    return found, lanes, mask


def contact_kernel(
    ids,
    count,
    recv,
    sides,
    disp,
    energy,
    mass,
    pair_node,
    pair_segment,
    pair_side,
    out,
    force,
    field,
    coords,
    nodes,
    picks,
):
    slave, node_lanes, node_mask = slave_places(disp, pair_node, nodes)
    row8 = iota((8, 128), 0)
    for i in range(NGX // 4):
        left, right = [], []
        for s in (4 * i, 4 * i + 2):
            even, odd = recv[s, 0:8].astype(f32), recv[s + 1, 0:8].astype(f32)
            left.append(jnp.where(row8 < 4, even, pltpu.roll(odd, 4, 0)))
            right.append(jnp.where(row8 < 4, pltpu.roll(even, 4, 0), odd))
        coords[16 * i : 16 * i + 16, 0:128] = jnp.concatenate(left, axis=0).astype(bf16)
        coords[16 * i : 16 * i + 16, 128:256] = jnp.concatenate(right, axis=0).astype(bf16)

    segment = pair_segment[...]
    ends = jnp.concatenate([segment, segment + 1], axis=1)
    lanes = one_hot(256, ends & 255)
    piece, line = ends >> 9, (ends >> 8) & 1
    looked = jnp.dot(coords[...], lanes, preferred_element_type=f32)
    level = [looked[8 * s : 8 * s + 8] for s in range(NGX // 2)]
    for bit in range(1, 5):
        upper = ((piece >> bit) & 1) == 1
        level = [jnp.where(upper, high, low) for low, high in zip(level[0::2], level[1::2])]
    found = level[0]
    row = iota((8, 2 * PAIRS), 0)
    at = (piece & 1) * 4 + line
    end_x = jnp.sum(jnp.where(row == at, found, 0.0), axis=0, keepdims=True)
    end_y = jnp.sum(jnp.where(row == at + 2, found, 0.0), axis=0, keepdims=True)

    live = iota((1, PAIRS), 1).astype(f32) < count[0:1, 0:1]
    push_x, push_y, magnitude, fraction = contact_terms(
        slave[0],
        slave[1],
        end_x[:, :PAIRS],
        end_y[:, :PAIRS],
        end_x[:, PAIRS:],
        end_y[:, PAIRS:],
        pair_side[...],
        live,
    )
    share = jnp.concatenate([1.0 - fraction, fraction], axis=1)
    terms = [share * jnp.concatenate([v, v], axis=1) for v in (-push_x, -push_y, magnitude)]
    stacked = jnp.where(row < 2, terms[0], jnp.where(row < 4, terms[1], terms[2]))
    stacked = jnp.where((row < 6) & ((row & 1) == line), stacked, 0.0)
    high, low = high_low(stacked)
    high = jnp.concatenate([high, high], axis=0).astype(bf16)
    low = jnp.concatenate([low, low], axis=0).astype(bf16)
    half = iota((16, 2 * PAIRS), 0) >> 3
    offset = (piece - half).astype(f32).astype(bf16)
    nothing = jnp.zeros((), bf16)
    for s in range(NGX // 2):
        mine = offset == jnp.asarray(2 * s, bf16)
        picks[16 * s : 16 * s + 16] = jnp.where(mine, high, nothing)
        picks[256 + 16 * s : 272 + 16 * s] = jnp.where(mine, low, nothing)
    contract = (((1,), (1,)), ((), ()))
    part = lax.dot_general(picks[...], lanes, contract, preferred_element_type=f32)
    reaction = part[0:256] + part[256:512]

    rows = [jnp.where(node_mask, half, 0.0) for v in (push_x, push_y) for half in high_low(v)]
    rows = jnp.concatenate([rows[0], rows[2], rows[1], rows[3]], axis=0).astype(bf16)
    part = lax.dot_general(rows, node_lanes, contract, preferred_element_type=f32)
    pushed = part[0:128] + part[128:256]

    least = zone_forces(ids, recv, sides, disp, energy, mass, field, force)
    for c in range(2):
        for h in range(2):
            at = 64 * c + 32 * h
            force[c, :, 128 * h : 128 * h + 128] += pushed[at : at + 32]
    row = iota((8, 256), 0)
    for s in range(NGX):
        out[s] = jnp.where(row == 6, least, reaction[8 * s : 8 * s + 8])


def sum_kernel(recv, chunk, out):
    total = recv[0]
    least = recv[0]
    for s in range(1, NGX):
        part = recv[s]
        total = total + part
        least = jnp.minimum(least, part)
    least = jnp.min(least[6:7], axis=1, keepdims=True)
    lane = iota((1, 128), 1)
    for z in range(NGY):
        rows = total[:, 128 * ((z % 8) // 4) : 128 * ((z % 8) // 4) + 128]
        line = jnp.broadcast_to(least, (1, 128))
        old = jnp.zeros((1, 128), f32)
        for c in range(3):
            shift = 32 * ((c - z) % 4)
            mine = (lane >= 32 * c) & (lane < 32 * c + 32)
            row = rows[2 * c + z // 8 : 2 * c + z // 8 + 1]
            line = jnp.where(mine, pltpu.roll(row, shift, 1) if shift else row, line)
            if c < 2:
                row = chunk[z // 4, 2 + c : 3 + c].astype(f32)
                old = jnp.where(mine, pltpu.roll(row, shift, 1) if shift else row, old)
        out[z, 0:1] = line
        out[z, 1:2] = old


def step_kernel(recv, force, vel, disp, mass, new_vel, new_disp, master):
    total = recv[0]
    least = recv[0]
    for z in range(1, NGY):
        part = recv[z]
        total = total + part
        least = jnp.minimum(least, part)
    lane = iota((1, 128), 1)
    least = jnp.where(lane >= 96, least[0:1], 1e30)
    step = 0.3 * jnp.min(least, axis=1, keepdims=True)
    for c in range(2):
        vel_c = vel[c] + step * force[c] / mass[...]
        new_vel[c] = vel_c
        new_disp[c] = disp[c] + step * vel_c
    moved = total[1:2] + step * total[0:1]
    for c in range(3):
        master[c : c + 1, :] = moved[:, 32 * c : 32 * c + 32]


def call(kernel, out, ins, scratch=(), flops=1_000_000):
    return pl.pallas_call(
        kernel,
        out_shape=[jax.ShapeDtypeStruct(s, d) for s, d in out],
        in_specs=[SMEM if i == "s" else VMEM for i in ins],
        out_specs=[VMEM] * len(out),
        scratch_shapes=[pltpu.VMEM(s, d) for s, d in scratch],
        compiler_params=pltpu.CompilerParams(vmem_limit_bytes=16 << 20),
        cost_estimate=pl.CostEstimate(flops=flops, bytes_accessed=1 << 20, transcendentals=0),
    )


def exchange(value, axes):
    return lax.all_to_all(value, axes, 0, 0, tiled=True)


def owner_piece(exchange, master_block, owner, count):
    tiles = master_block[0].reshape(4, NGX, 4, 128).transpose(1, 2, 0, 3)
    out = [((4, 4, 128), bf16), ((8, 128), f32)]

    def send(tiles, owner, count):
        recv = exchange(tiles, GX)
        tile, at = call(tile_kernel, [out[1], ((8, 128), jnp.int32)], "ss", flops=100_000_000)(owner, count)
        return call(pick_kernel, out[:1], "vv")(at, recv)[0], tile

    def idle(tiles, owner, count):
        return tuple(call(idle_kernel, out, "s")(count))

    mine = lax.axis_index("gy") == (owner[0] & (NGY - 1))
    return lax.cond(mine, send, idle, tiles, owner, count)


def stages(
    exchange,
    node_disp,
    node_vel,
    node_mass,
    zone_mass,
    zone_energy,
    master_block,
    owner,
    pair_node,
    pair_segment,
    pair_side,
    pair_count,
):
    fields = (node_disp, zone_energy, zone_mass)
    chunk, count = owner_piece(exchange, master_block, owner, pair_count)
    (sent,) = call(spread_kernel, [((NGY, 3, 4, 128), bf16)], "vvvv")(chunk, *fields)
    sent = exchange(sent, "gy")
    sent, sides = call(gather_kernel, [((NGX, 16, 128), bf16), ((8, 128), f32)], "svvvv")(
        owner, sent, *fields
    )
    sent = exchange(sent, GX)
    sent, force = call(
        contact_kernel,
        [((NGX, 8, 256), f32), ((2, ROWS, COLS), f32)],
        "svvvvvvvvv",
        [
            ((3, ROWS + 8, COLS + 128), f32),
            ((128, 256), bf16),
            ((384, 128), bf16),
            ((512, 2 * PAIRS), bf16),
        ],
    )(owner, count, sent, sides, *fields, pair_node, pair_segment, pair_side)
    sent = exchange(sent, GX)
    (sent,) = call(sum_kernel, [((NGY, 2, 128), f32)], "vv")(sent, chunk)
    sent = exchange(sent, "gy")
    return tuple(
        call(
            step_kernel,
            [((2, ROWS, COLS), f32), ((2, ROWS, COLS), f32), ((3, 32), f32)],
            "vvvvv",
        )(sent, force, node_vel, node_disp, node_mass)
    )


def shards(*args):
    return stages(exchange, *args)


def solution(mesh):
    split = Mesh(mesh.devices.reshape(4, 4, 2, mesh.shape["gy"]), ("gx_0", "gx_1", "gx_2", "gy"))
    in_specs = (
        P(None, GX, "gy"),
        P(None, GX, "gy"),
        P(GX, "gy"),
        P(GX, "gy"),
        P(GX, "gy"),
        P(GX_GY, None, None),
        P(),
        P(GX_GY, None),
        P(GX_GY, None),
        P(GX_GY, None),
        P(GX_GY),
    )
    out_specs = (P(None, GX, "gy"), P(None, GX, "gy"), P(None, GX_GY))
    return jax.shard_map(
        shards, mesh=split, in_specs=in_specs, out_specs=out_specs, check_vma=False
    )
```

```python
import jax
import jax.numpy as jnp
from jax import lax
from jax.experimental import pallas as pl
from jax.experimental.pallas import tpu as pltpu
from jax.sharding import Mesh
from jax.sharding import PartitionSpec as P

GX = ("gx_0", "gx_1", "gx_2")
GX_GY = ("gx_0", "gx_1", "gx_2", "gy")
NGX = 32
NGY = 16
ROWS = 32
COLS = 256
PAIRS = 1024
TOTAL_ROWS = NGX * ROWS
TOTAL_COLS = NGY * COLS
STIFFNESS = 10.0
GAP_SCALE = 0.05

f32 = jnp.float32
bf16 = jnp.bfloat16
VMEM = pl.BlockSpec(memory_space=pltpu.VMEM)
SMEM = pl.BlockSpec(memory_space=pltpu.SMEM)


def place(ids):
    return ids[0], lax.axis_index(GX), lax.axis_index("gy")


def iota(shape, dim):
    return lax.broadcasted_iota(jnp.int32, shape, dim)


def rows_of(pieces):
    row = iota((8, 128), 0)
    tile = jnp.zeros((8, 128), f32)
    for k, piece in enumerate(pieces):
        tile = jnp.where(row == k, piece, tile)
    return tile


def column_row(columns):
    line, lane = iota((ROWS, 128), 0), iota((ROWS, 128), 1)
    out = jnp.zeros((ROWS, 128), f32)
    for c, column in enumerate(columns):
        out = jnp.where(lane == line + 32 * c, column, out)
    return jnp.sum(out, axis=0, keepdims=True)


def count_tile(count):
    return jnp.full((8, 128), count[0].astype(f32))


def tile_kernel(owner, count, tile, at):
    tile[...] = count_tile(count)
    at[...] = jnp.full((8, 128), owner[0] // NGY)


def pick_kernel(at, recv, chunk):
    picked = jnp.zeros((4, 4, 128), f32)
    for s in range(NGX):
        picked = jnp.where((at[0:4] == s)[None], recv[s].astype(f32), picked)
    chunk[...] = picked.astype(bf16)


def idle_kernel(count, chunk, tile):
    chunk[...] = jnp.zeros((4, 4, 128), bf16)
    tile[...] = count_tile(count)


def spread_kernel(chunk, disp, energy, mass, out):
    for h in range(2):
        rows = [chunk[2 * r + h, c : c + 1].astype(f32) for c in range(2) for r in range(2)]
        coords = rows_of(rows)[0:4].astype(bf16)
        for z in range(NGY):
            out[z, h] = coords

    def edge(at):
        cut = slice(at, at + 1)
        columns = [disp[0, :, cut], disp[1, :, cut], energy[:, cut] * mass[:, cut]]
        return rows_of([column_row(columns)])[0:4].astype(bf16)

    head, tail = edge(0), edge(COLS - 1)
    for z in range(NGY):
        out[z, 2] = head
    out[lax.rem(lax.axis_index("gy") + 1, NGY), 2] = tail


def gather_kernel(ids, recv, disp, energy, mass, out, sides):
    owner, gx, gy = place(ids)
    picked = recv[lax.rem(owner, NGY)].astype(f32)
    left = recv[lax.rem(gy + NGY - 1, NGY), 2].astype(f32)[0:1]
    right = recv[lax.rem(gy + 1, NGY), 2].astype(f32)[0:1]
    coords = jnp.concatenate([picked[0], picked[1]], axis=0)
    sides[...] = rows_of([left, right])

    def edge(at):
        cut = slice(at, at + 1)
        fields = (disp[0, cut], disp[1, cut], energy[cut] * mass[cut])
        return rows_of([f[:, h : h + 128] for f in fields for h in (0, 128)] + [left, right])

    tail = jnp.concatenate([coords, edge(ROWS - 1)], axis=0).astype(bf16)
    head = jnp.concatenate([coords, edge(0)], axis=0).astype(bf16)
    for d in range(NGX):
        out[d] = head
    out[lax.rem(gx + 1, NGX)] = tail


def zone_forces(ids, recv, sides, disp, energy, mass, field, force):
    _, gx, gy = place(ids)
    above = recv[lax.rem(gx + NGX - 1, NGX)].astype(f32)[8:16]
    below = recv[lax.rem(gx + 1, NGX)].astype(f32)[8:16]
    row8, lane8 = iota((8, 128), 0), iota((8, 128), 1)
    line, lane = iota((ROWS, 128), 0), iota((ROWS, 128), 1)
    lane1 = iota((1, 128), 1)

    def corner(rows, k, at):
        return jnp.sum(jnp.where(lane1 == at, rows[k : k + 1], 0.0), axis=1, keepdims=True)

    for c in range(3):
        own = energy[...] * mass[...] if c == 2 else disp[c]
        field[c, 0:ROWS, 0:COLS] = own
        for h in range(2):
            k = 2 * c + h
            field[c, ROWS : ROWS + 8, 128 * h : 128 * h + 128] = jnp.where(
                row8 == 0, below[k : k + 1], jnp.where(row8 == 7, above[k : k + 1], 0.0)
            )
        cols = [
            jnp.sum(jnp.where(lane == line + 32 * c, sides[k : k + 1], 0.0), axis=1, keepdims=True)
            for k in range(2)
        ]
        field[c, 0:ROWS, COLS : COLS + 128] = jnp.where(
            lane == 0, cols[1], jnp.where(lane == 127, cols[0], 0.0)
        )
        first, last = 32 * c, 32 * c + 31
        low = jnp.where(
            lane8 == 0, corner(below, 7, first), jnp.where(lane8 == 127, corner(below, 6, first), 0.0)
        )
        high = jnp.where(
            lane8 == 0, corner(above, 7, last), jnp.where(lane8 == 127, corner(above, 6, last), 0.0)
        )
        field[c, ROWS : ROWS + 8, COLS : COLS + 128] = jnp.where(
            row8 == 0, low, jnp.where(row8 == 7, high, 0.0)
        )

    height, width = ROWS + 8, COLS + 128

    def next_row(v):
        return pltpu.roll(v, height - 1, 0)

    def next_col(v):
        return pltpu.roll(v, width - 1, 1)

    def prev_row(v):
        return pltpu.roll(v, 1, 0)

    def prev_col(v):
        return pltpu.roll(v, 1, 1)

    first, second = [], []
    for c in range(2):
        a = field[c]
        b = next_row(a)
        first.append(next_col(b) - a + 1.0)
        second.append(next_col(a) - b + (-1.0 if c == 0 else 1.0))
    at_row, at_col = iota((height, width), 0), iota((height, width), 1)
    zone_row = jnp.where(at_row == height - 1, -1, at_row)
    zone_col = jnp.where(at_col == width - 1, -1, at_col)
    in_row, in_col = gx * ROWS + zone_row, gy * COLS + zone_col
    live = (
        (zone_row < ROWS)
        & (zone_col < COLS)
        & (in_row >= 0)
        & (in_row < TOTAL_ROWS - 1)
        & (in_col >= 0)
        & (in_col < TOTAL_COLS - 1)
    )
    area = jnp.where(live, 0.5 * (first[0] * second[1] - second[0] * first[1]), 1.0)
    press = jnp.where(live, 0.2 * field[2] / area, 0.0)
    on_a = (-press * second[1], press * second[0])
    on_b = (press * first[1], -press * first[0])
    for c in range(2):
        total = (on_a[c] - prev_col(on_b[c])) + prev_row(on_b[c] - prev_col(on_a[c]))
        force[c] = total[0:ROWS, 0:COLS]
    scale = jnp.where(
        live[0:ROWS, 0:COLS], jnp.sqrt(area[0:ROWS, 0:COLS]) / jnp.sqrt(0.56 * energy[...]), 1e30
    )
    return jnp.min(scale, axis=0, keepdims=True)


def contact_terms(slave_x, slave_y, start_x, start_y, end_x, end_y, side, live):
    rel_x = slave_x - start_x + 0.5
    rel_y = slave_y - start_y
    along_x = 1.0 + end_x - start_x
    along_y = end_y - start_y
    along_sq = along_x * along_x + along_y * along_y
    length = jnp.sqrt(along_sq)
    fraction = (rel_x * along_x + rel_y * along_y) / along_sq
    normal_x = -along_y / length
    normal_y = along_x / length
    gap_size = normal_x * rel_x + normal_y * rel_y
    sign = 1.0 - 2.0 * side.astype(f32)
    depth = -sign * gap_size / GAP_SCALE
    soft = jnp.maximum(depth, 0.0) + jnp.log1p(jnp.exp(-jnp.abs(depth)))
    magnitude = jnp.where(live, STIFFNESS * GAP_SCALE * soft, 0.0)
    return magnitude * sign * normal_x, magnitude * sign * normal_y, magnitude, fraction


def high_low(v):
    high = v.astype(bf16).astype(f32)
    return high, v - high


def one_hot(count, index):
    at = lax.broadcasted_iota(jnp.int32, (count, index.shape[1]), 0).astype(f32).astype(bf16)
    return jnp.where(at == index.astype(f32).astype(bf16), jnp.ones((), bf16), jnp.zeros((), bf16))


def node_place(node):
    row = ((node >> 7) & 1) * 32 + (node >> 8)
    return one_hot(128, node & 127), iota((64, PAIRS), 0) == row


def slave_places(disp, pair_node, nodes):
    for c in range(2):
        for h in range(2):
            rest = disp[c, :, 128 * h : 128 * h + 128]
            for k in range(3):
                high, low = high_low(rest)
                at = 128 * k + 64 * c + 32 * h
                nodes[at : at + 32] = high.astype(bf16)
                rest = low
    lanes, mask = node_place(pair_node[...])
    seen = jnp.dot(nodes[...], lanes, preferred_element_type=f32)
    seen = (seen[256:384] + seen[128:256]) + seen[0:128]
    row = ((pair_node[...] >> 7) & 1) * 32 + (pair_node[...] >> 8)
    found = []
    for c in range(2):
        level = [seen[64 * c + 8 * g : 64 * c + 8 * g + 8] for g in range(8)]
        for bit in range(3, 6):
            upper = ((row >> bit) & 1) == 1
            level = [jnp.where(upper, high, low) for low, high in zip(level[0::2], level[1::2])]
        one = jnp.where(iota((8, PAIRS), 0) == (row & 7), level[0], 0.0)
        found.append(jnp.sum(one, axis=0, keepdims=True))
    return found, lanes, mask


def contact_kernel(
    ids,
    count,
    recv,
    sides,
    disp,
    energy,
    mass,
    pair_node,
    pair_segment,
    pair_side,
    out,
    force,
    field,
    coords,
    nodes,
    picks,
):
    slave, node_lanes, node_mask = slave_places(disp, pair_node, nodes)
    row8 = iota((8, 128), 0)
    for i in range(NGX // 4):
        left, right = [], []
        for s in (4 * i, 4 * i + 2):
            even, odd = recv[s, 0:8].astype(f32), recv[s + 1, 0:8].astype(f32)
            left.append(jnp.where(row8 < 4, even, pltpu.roll(odd, 4, 0)))
            right.append(jnp.where(row8 < 4, pltpu.roll(even, 4, 0), odd))
        coords[16 * i : 16 * i + 16, 0:128] = jnp.concatenate(left, axis=0).astype(bf16)
        coords[16 * i : 16 * i + 16, 128:256] = jnp.concatenate(right, axis=0).astype(bf16)

    segment = pair_segment[...]
    ends = jnp.concatenate([segment, segment + 1], axis=1)
    lanes = one_hot(256, ends & 255)
    piece, line = ends >> 9, (ends >> 8) & 1
    looked = jnp.dot(coords[...], lanes, preferred_element_type=f32)
    level = [looked[8 * s : 8 * s + 8] for s in range(NGX // 2)]
    for bit in range(1, 5):
        upper = ((piece >> bit) & 1) == 1
        level = [jnp.where(upper, high, low) for low, high in zip(level[0::2], level[1::2])]
    found = level[0]
    row = iota((8, 2 * PAIRS), 0)
    at = (piece & 1) * 4 + line
    end_x = jnp.sum(jnp.where(row == at, found, 0.0), axis=0, keepdims=True)
    end_y = jnp.sum(jnp.where(row == at + 2, found, 0.0), axis=0, keepdims=True)

    live = iota((1, PAIRS), 1).astype(f32) < count[0:1, 0:1]
    push_x, push_y, magnitude, fraction = contact_terms(
        slave[0],
        slave[1],
        end_x[:, :PAIRS],
        end_y[:, :PAIRS],
        end_x[:, PAIRS:],
        end_y[:, PAIRS:],
        pair_side[...],
        live,
    )
    share = jnp.concatenate([1.0 - fraction, fraction], axis=1)
    terms = [share * jnp.concatenate([v, v], axis=1) for v in (-push_x, -push_y, magnitude)]
    stacked = jnp.where(row < 2, terms[0], jnp.where(row < 4, terms[1], terms[2]))
    stacked = jnp.where((row < 6) & ((row & 1) == line), stacked, 0.0)
    high, low = high_low(stacked)
    high = jnp.concatenate([high, high], axis=0).astype(bf16)
    low = jnp.concatenate([low, low], axis=0).astype(bf16)
    half = iota((16, 2 * PAIRS), 0) >> 3
    offset = (piece - half).astype(f32).astype(bf16)
    nothing = jnp.zeros((), bf16)
    for s in range(NGX // 2):
        mine = offset == jnp.asarray(2 * s, bf16)
        picks[16 * s : 16 * s + 16] = jnp.where(mine, high, nothing)
        picks[256 + 16 * s : 272 + 16 * s] = jnp.where(mine, low, nothing)
    contract = (((1,), (1,)), ((), ()))
    part = lax.dot_general(picks[...], lanes, contract, preferred_element_type=f32)
    reaction = part[0:256] + part[256:512]

    rows = [jnp.where(node_mask, half, 0.0) for v in (push_x, push_y) for half in high_low(v)]
    rows = jnp.concatenate([rows[0], rows[2], rows[1], rows[3]], axis=0).astype(bf16)
    part = lax.dot_general(rows, node_lanes, contract, preferred_element_type=f32)
    pushed = part[0:128] + part[128:256]

    least = zone_forces(ids, recv, sides, disp, energy, mass, field, force)
    for c in range(2):
        for h in range(2):
            at = 64 * c + 32 * h
            force[c, :, 128 * h : 128 * h + 128] += pushed[at : at + 32]
    row = iota((8, 256), 0)
    for s in range(NGX):
        out[s] = jnp.where(row == 6, least, reaction[8 * s : 8 * s + 8])


def sum_kernel(recv, chunk, out):
    total = recv[0]
    least = recv[0]
    for s in range(1, NGX):
        part = recv[s]
        total = total + part
        least = jnp.minimum(least, part)
    least = jnp.min(least[6:7], axis=1, keepdims=True)
    lane = iota((1, 128), 1)
    for z in range(NGY):
        rows = total[:, 128 * ((z % 8) // 4) : 128 * ((z % 8) // 4) + 128]
        line = jnp.broadcast_to(least, (1, 128))
        old = jnp.zeros((1, 128), f32)
        for c in range(3):
            shift = 32 * ((c - z) % 4)
            mine = (lane >= 32 * c) & (lane < 32 * c + 32)
            row = rows[2 * c + z // 8 : 2 * c + z // 8 + 1]
            line = jnp.where(mine, pltpu.roll(row, shift, 1) if shift else row, line)
            if c < 2:
                row = chunk[z // 4, 2 + c : 3 + c].astype(f32)
                old = jnp.where(mine, pltpu.roll(row, shift, 1) if shift else row, old)
        out[z, 0:1] = line
        out[z, 1:2] = old


def step_kernel(recv, force, vel, disp, mass, new_vel, new_disp, master):
    total = recv[0]
    least = recv[0]
    for z in range(1, NGY):
        part = recv[z]
        total = total + part
        least = jnp.minimum(least, part)
    lane = iota((1, 128), 1)
    least = jnp.where(lane >= 96, least[0:1], 1e30)
    step = 0.3 * jnp.min(least, axis=1, keepdims=True)
    for c in range(2):
        vel_c = vel[c] + step * force[c] / mass[...]
        new_vel[c] = vel_c
        new_disp[c] = disp[c] + step * vel_c
    moved = total[1:2] + step * total[0:1]
    for c in range(3):
        master[c : c + 1, :] = moved[:, 32 * c : 32 * c + 32]


def call(kernel, out, ins, scratch=(), flops=1_000_000):
    return pl.pallas_call(
        kernel,
        out_shape=[jax.ShapeDtypeStruct(s, d) for s, d in out],
        in_specs=[SMEM if i == "s" else VMEM for i in ins],
        out_specs=[VMEM] * len(out),
        scratch_shapes=[pltpu.VMEM(s, d) for s, d in scratch],
        compiler_params=pltpu.CompilerParams(vmem_limit_bytes=16 << 20),
        cost_estimate=pl.CostEstimate(flops=flops, bytes_accessed=1 << 20, transcendentals=0),
    )


def exchange(value, axes):
    return lax.all_to_all(value, axes, 0, 0, tiled=True)


def owner_piece(exchange, master_block, owner, count):
    tiles = master_block[0].reshape(4, NGX, 4, 128).transpose(1, 2, 0, 3)
    out = [((4, 4, 128), bf16), ((8, 128), f32)]

    def send(tiles, owner, count):
        recv = exchange(tiles, GX)
        tile, at = call(tile_kernel, [out[1], ((8, 128), jnp.int32)], "ss", flops=100_000_000)(owner, count)
        return call(pick_kernel, out[:1], "vv")(at, recv)[0], tile

    def idle(tiles, owner, count):
        return tuple(call(idle_kernel, out, "s")(count))

    mine = lax.axis_index("gy") == (owner[0] & (NGY - 1))
    return lax.cond(mine, send, idle, tiles, owner, count)


def stages(
    exchange,
    node_disp,
    node_vel,
    node_mass,
    zone_mass,
    zone_energy,
    master_block,
    owner,
    pair_node,
    pair_segment,
    pair_side,
    pair_count,
):
    fields = (node_disp, zone_energy, zone_mass)
    chunk, count = owner_piece(exchange, master_block, owner, pair_count)
    (sent,) = call(spread_kernel, [((NGY, 3, 4, 128), bf16)], "vvvv")(chunk, *fields)
    sent = exchange(sent, "gy")
    sent, sides = call(gather_kernel, [((NGX, 16, 128), bf16), ((8, 128), f32)], "svvvv")(
        owner, sent, *fields
    )
    sent = exchange(sent, GX)
    sent, force = call(
        contact_kernel,
        [((NGX, 8, 256), f32), ((2, ROWS, COLS), f32)],
        "svvvvvvvvv",
        [
            ((3, ROWS + 8, COLS + 128), f32),
            ((128, 256), bf16),
            ((384, 128), bf16),
            ((512, 2 * PAIRS), bf16),
        ],
    )(owner, count, sent, sides, *fields, pair_node, pair_segment, pair_side)
    sent = exchange(sent, GX)
    (sent,) = call(sum_kernel, [((NGY, 2, 128), f32)], "vv")(sent, chunk)
    sent = exchange(sent, "gy")
    return tuple(
        call(
            step_kernel,
            [((2, ROWS, COLS), f32), ((2, ROWS, COLS), f32), ((3, 32), f32)],
            "vvvvv",
        )(sent, force, node_vel, node_disp, node_mass)
    )


def shards(*args):
    return stages(exchange, *args)


def solution(mesh):
    split = Mesh(mesh.devices.reshape(4, 4, 2, mesh.shape["gy"]), ("gx_0", "gx_1", "gx_2", "gy"))
    in_specs = (
        P(None, GX, "gy"),
        P(None, GX, "gy"),
        P(GX, "gy"),
        P(GX, "gy"),
        P(GX, "gy"),
        P(GX_GY, None, None),
        P(),
        P(GX_GY, None),
        P(GX_GY, None),
        P(GX_GY, None),
        P(GX_GY),
    )
    out_specs = (P(None, GX, "gy"), P(None, GX, "gy"), P(None, GX_GY))
    return jax.shard_map(
        shards, mesh=split, in_specs=in_specs, out_specs=out_specs, check_vma=False
    )
```
